512 devices in a mesh: seq: 256 (over z, x, y_lo, core), head: 2 (over y_hi).
Axes of the slice: x: 4, y: 8 (y_hi: 2, y_lo: 4; y = y_hi * 4 + y_lo), z: 8, core: 2. Of those that a mesh axis runs over, the one named last changes fastest.
Arguments:
- queries: bfloat16 [32768, 2048], P('seq', 'head'), may hold values from -5 to 5
- keys: bfloat16 [32768, 2048], P('seq', 'head'), may hold values from -5 to 5
- values: bfloat16 [32768, 2048], P('seq', 'head'), may hold values from -6 to 6
- grad_out: bfloat16 [32768, 2048], P('seq', 'head'), may hold values from -6 to 6
- doc_ids: int32 [32768], P(('seq', 'head')), may hold values from 0 to 511, never falling along the last dimension, each value on 1 to 512 neighbouring positions
- loss_mask: int32 [32768], P(('seq', 'head')), may hold values 0 or 1
Outputs:
- attended: bfloat16 [32768, 2048], P('seq', 'head')
- query_grad: bfloat16 [32768, 2048], P('seq', 'head')
- key_grad: bfloat16 [32768, 2048], P('seq', 'head')
- value_grad: bfloat16 [32768, 2048], P('seq', 'head')
The draws below stay inside these ranges and needn't reach their ends.
Inputs may be any that keep to these rules, and one draw needn't show every extreme that they name: `doc_ids`: documents are runs of consecutive tokens numbered 0, 1, 2, ... in order; each has 1 to 512 tokens.
All inputs are finite; a program needn't handle non-finite values. No bound on the sum of `loss_mask` on one device may be relied on, other than what follows from the above.
Results may differ from the reference program's by a relative error of at most 0.033.
Values may be sent and summed in bfloat16 or wider, within the bound.
A program may use at most 64 MiB of HBM per device.

```python
import math
import jax
import jax.numpy as jnp
import numpy as np
from jax import lax

TOK_DEV = 128
HEAD_DIM = 128
HEADS = 16
WINDOW = 512
TOKENS = 32768
DOCS = 512
MOST_DOC = 512
N_SEQ = 256


def shared_pair(key):
    width = HEADS * HEAD_DIM
    key_query = jax.random.fold_in(key, 101)
    key_key = jax.random.fold_in(key, 102)
    query_rows = jnp.clip(jax.random.normal(key_query, (TOKENS, width), jnp.float32), -5.0, 5.0)
    key_rows = jnp.clip(jax.random.normal(key_key, (TOKENS, width), jnp.float32), -5.0, 5.0)
    return (query_rows.astype(jnp.bfloat16), key_rows.astype(jnp.bfloat16))


def draw_queries(key, part):
    return shared_pair(key)[0]


def draw_keys(key, part):
    return shared_pair(key)[1]


def set_ends(drawn, stream_key, low, high):
    longest = drawn.shape.index(max(drawn.shape))
    spots = []
    for shift in (0, 1):
        where = [jax.random.randint(jax.random.fold_in(stream_key, axis), (), 0, length) for axis, length in enumerate(drawn.shape)]
        where[longest] = (where[longest] + shift) % drawn.shape[longest]
        spots.append(tuple(where))
    return drawn.at[spots[0]].set(low).at[spots[1]].set(high)


def level_of(rng, dims, pieces, low, largest):
    def one(position, parts):
        heights = jax.random.uniform(jax.random.fold_in(jax.random.fold_in(rng, 6), position), (parts,), jnp.float32, low / len(pieces), largest / len(pieces))
        return jnp.repeat(jnp.exp(heights), dims[position] // parts).reshape((-1,) + (1,) * (len(dims) - position - 1))

    loudness = one(*pieces[0])
    for cut in pieces[1:]:
        loudness = loudness * one(*cut)
    return loudness


def profile(number_of, total, reach, skew):
    loads = [(1 << 20) // math.isqrt(standing ** skew) + 1 for standing in range(2, number_of + 1)]
    spare, given = total - reach - (number_of - 1), [1] * (number_of - 1)
    while spare > 0:
        free = [i for i in range(number_of - 1) if given[i] < reach]
        whole, budget = sum([loads[i] for i in free]), spare
        for i in free:
            addition = min(reach - given[i], max(1, budget * loads[i] // whole), spare)
            given[i] = given[i] + addition
            spare = spare - addition
    return np.array([reach] + given)


def uneven_parts(stream_key, amount, total, reach, lean):
    if amount == 2:
        one = jax.random.randint(stream_key, (), max(1, total - reach), min(reach, total - 1) + 1)
        return jnp.stack([one, total - one])
    tallies = jnp.asarray(profile(amount, total, reach, lean), jnp.int32)
    pairs = (amount - 1) // 2
    giver, sink = tallies[1:1 + 2 * pairs:2], tallies[2:2 + 2 * pairs:2]
    slack = jnp.minimum(giver - 1, reach - sink)
    passed = jax.random.randint(jax.random.fold_in(stream_key, 1), (pairs,), 0, 1 << 20) % (slack + 1)
    tallies = tallies.at[1:1 + 2 * pairs:2].set(giver - passed).at[2:2 + 2 * pairs:2].set(sink + passed)
    return tallies[jax.random.permutation(jax.random.fold_in(stream_key, 2), amount)]


def gaussian(rng, shape, deviation, reach, shards=(), kind=jnp.bfloat16):
    drawn = jax.random.normal(rng, shape, jnp.float32) * deviation
    if len(shards) > 0:
        drawn = level_of(rng, shape, shards, -0.22, 0.18) * drawn
    return jnp.clip(drawn, min=-reach, max=reach).astype(kind)


def setup_inputs(seed: int = 0) -> dict:
    seeds = jax.random.split(jax.random.key(seed), 7)
    return {
        "queries": draw_queries(jax.random.fold_in(seeds[6], 71), 0),
        "keys": draw_keys(jax.random.fold_in(seeds[6], 71), 0),
        "values": gaussian(seeds[2], (TOKENS, HEADS * HEAD_DIM), 1.0, 6.0, ((0, 256), (1, 2))),
        "grad_out": gaussian(seeds[3], (TOKENS, HEADS * HEAD_DIM), 1.0, 6.0, ((0, 256), (1, 2))),
        "doc_ids": jnp.searchsorted(jnp.cumsum(uneven_parts(seeds[4], DOCS, TOKENS, MOST_DOC, 2)), jnp.arange(TOKENS), side="right").astype(jnp.int32),
        "loss_mask": set_ends((jax.random.randint(seeds[5], (TOKENS,), 0, 4) < 3).astype(jnp.int32), jax.random.fold_in(seeds[5], 1), 0, 1),
    }


masked_value = -1e+30

def rounded(values_in):
    return lax.optimization_barrier(values_in.astype(jnp.bfloat16)).astype(jnp.float32)

def by_head(rows):
    return rows.astype(jnp.float32).reshape(rows.shape[0], -1, HEAD_DIM)

def masked_scores(q_rows, k_rows, q_pos, k_pos, q_start):
    score = jnp.einsum('qhd,khd->hqk', by_head(q_rows), by_head(k_rows)) * (1.0 / math.sqrt(HEAD_DIM))
    later = k_pos[None, :] <= q_pos[:, None]
    inside = k_pos[None, :] > q_pos[:, None] - WINDOW
    same_doc = k_pos[None, :] >= q_start[:, None]
    return jnp.where((later & inside & same_doc)[None], score, masked_value)

def reference(queries, keys, values, grad_out, doc_ids, loss_mask):
    width = queries.shape[1]
    head_count = width // HEAD_DIM
    scaling = 1.0 / math.sqrt(HEAD_DIM)
    positions = jnp.arange(TOKENS, dtype=jnp.int32)
    change = jnp.concatenate([jnp.ones((1,), dtype=bool), doc_ids[1:] != doc_ids[:-1]])
    doc_start = lax.cummax(jnp.where(change, positions, 0), axis=0).astype(jnp.int32)
    counts = jax.ops.segment_sum(loss_mask.astype(jnp.float32), doc_ids, num_segments=DOCS)
    weight = loss_mask.astype(jnp.float32) * TOK_DEV / jnp.maximum(counts[doc_ids], TOK_DEV // 8)
    padding = jnp.zeros((WINDOW, width), queries.dtype)
    keys_left = jnp.concatenate([padding, keys])
    values_left = jnp.concatenate([padding, values])
    block_ids = jnp.arange(N_SEQ, dtype=jnp.int32)

    def forward(block_id):
        first_row = block_id * TOK_DEV
        q_rows = lax.dynamic_slice_in_dim(queries, first_row, TOK_DEV, 0)
        k_rows = lax.dynamic_slice_in_dim(keys_left, first_row, TOK_DEV + WINDOW, 0)
        v_rows = lax.dynamic_slice_in_dim(values_left, first_row, TOK_DEV + WINDOW, 0)
        q_pos = first_row + jnp.arange(TOK_DEV, dtype=jnp.int32)
        k_pos = first_row - WINDOW + jnp.arange(TOK_DEV + WINDOW, dtype=jnp.int32)
        q_start = lax.dynamic_slice_in_dim(doc_start, first_row, TOK_DEV, 0)
        score = masked_scores(q_rows, k_rows, q_pos, k_pos, q_start)
        row_max = lax.optimization_barrier(jnp.max(score, axis=2))
        log_block = row_max + jnp.log(lax.optimization_barrier(jnp.sum(jnp.exp(score - row_max[..., None]), axis=2)))
        prob = jnp.exp(score - log_block[..., None])
        mixed = jnp.einsum('hqk,khd->qhd', rounded(prob), by_head(v_rows))
        return (mixed.reshape(TOK_DEV, width).astype(jnp.bfloat16), log_block)
    out_blocks, log_blocks = lax.map(forward, block_ids)
    attended = lax.optimization_barrier(out_blocks.reshape(TOKENS, width))
    log_total = jnp.transpose(log_blocks, (1, 0, 2)).reshape(head_count, TOKENS)
    grad_rows = lax.optimization_barrier((weight[:, None] * grad_out.astype(jnp.float32)).astype(jnp.bfloat16))
    row_delta = lax.optimization_barrier(jnp.sum(by_head(grad_rows) * by_head(attended), axis=2)).T

    def query_side(block_id):
        first_row = block_id * TOK_DEV
        q_rows = lax.dynamic_slice_in_dim(queries, first_row, TOK_DEV, 0)
        g_rows = lax.dynamic_slice_in_dim(grad_rows, first_row, TOK_DEV, 0)
        k_rows = lax.dynamic_slice_in_dim(keys_left, first_row, TOK_DEV + WINDOW, 0)
        v_rows = lax.dynamic_slice_in_dim(values_left, first_row, TOK_DEV + WINDOW, 0)
        q_pos = first_row + jnp.arange(TOK_DEV, dtype=jnp.int32)
        k_pos = first_row - WINDOW + jnp.arange(TOK_DEV + WINDOW, dtype=jnp.int32)
        q_start = lax.dynamic_slice_in_dim(doc_start, first_row, TOK_DEV, 0)
        log_block = lax.dynamic_slice_in_dim(log_total, first_row, TOK_DEV, 1)
        delta_block = lax.dynamic_slice_in_dim(row_delta, first_row, TOK_DEV, 1)
        score = masked_scores(q_rows, k_rows, q_pos, k_pos, q_start)
        prob = jnp.exp(score - log_block[..., None])
        prob_grad = jnp.einsum('qhd,khd->hqk', by_head(g_rows), by_head(v_rows))
        score_grad = rounded(prob * (prob_grad - delta_block[..., None]) * scaling)
        result = jnp.einsum('hqk,khd->qhd', score_grad, by_head(k_rows))
        return result.reshape(TOK_DEV, width).astype(jnp.bfloat16)
    query_grad = lax.map(query_side, block_ids).reshape(TOKENS, width)
    q_right = jnp.concatenate([queries, padding])
    g_right = jnp.concatenate([grad_rows, padding.astype(grad_rows.dtype)])
    log_right = jnp.concatenate([log_total, jnp.zeros((head_count, WINDOW), jnp.float32)], axis=1)
    delta_right = jnp.concatenate([row_delta, jnp.zeros((head_count, WINDOW), jnp.float32)], axis=1)
    start_right = jnp.concatenate([doc_start, jnp.full((WINDOW,), TOKENS, jnp.int32)])

    def key_side(block_id):
        first_row = block_id * TOK_DEV
        k_rows = lax.dynamic_slice_in_dim(keys, first_row, TOK_DEV, 0)
        v_rows = lax.dynamic_slice_in_dim(values, first_row, TOK_DEV, 0)
        q_rows = lax.dynamic_slice_in_dim(q_right, first_row, TOK_DEV + WINDOW, 0)
        g_rows = lax.dynamic_slice_in_dim(g_right, first_row, TOK_DEV + WINDOW, 0)
        log_block = lax.dynamic_slice_in_dim(log_right, first_row, TOK_DEV + WINDOW, 1)
        delta_block = lax.dynamic_slice_in_dim(delta_right, first_row, TOK_DEV + WINDOW, 1)
        q_start = lax.dynamic_slice_in_dim(start_right, first_row, TOK_DEV + WINDOW, 0)
        q_pos = first_row + jnp.arange(TOK_DEV + WINDOW, dtype=jnp.int32)
        k_pos = first_row + jnp.arange(TOK_DEV, dtype=jnp.int32)
        score = masked_scores(q_rows, k_rows, q_pos, k_pos, q_start)
        prob = jnp.exp(score - log_block[..., None])
        prob_grad = jnp.einsum('qhd,khd->hqk', by_head(g_rows), by_head(v_rows))
        score_grad = rounded(prob * (prob_grad - delta_block[..., None]) * scaling)
        key_part = jnp.einsum('hqk,qhd->khd', score_grad, by_head(q_rows))
        value_part = jnp.einsum('hqk,qhd->khd', rounded(prob), by_head(g_rows))
        return (key_part.reshape(TOK_DEV, width).astype(jnp.bfloat16), value_part.reshape(TOK_DEV, width).astype(jnp.bfloat16))
    key_blocks, value_blocks = lax.map(key_side, block_ids)
    return (attended, query_grad, key_blocks.reshape(TOKENS, width), value_blocks.reshape(TOKENS, width))
```

```python
import functools
import math

import jax
import jax.numpy as jnp
from jax import lax
from jax.experimental import pallas as pl
from jax.experimental.pallas import tpu as pltpu
from jax.sharding import PartitionSpec as P

HEAD_DIM = 128
MASKED = -1e30
SCALE = 1.0 / math.sqrt(HEAD_DIM)
MESH = pl.DeviceIdType.MESH
NN = (((1,), (0,)), ((), ()))
NT = (((1,), (1,)), ((), ()))
TN = (((0,), (0,)), ((), ()))


def dot(a, b, dims):
    return lax.dot_general(a, b, dims, preferred_element_type=jnp.float32)


def kernel(
    n_chip,
    rows,
    heads,
    q_in,
    k_in,
    v_in,
    g_in,
    ids_in,
    mask_in,
    o_out,
    qg_out,
    kg_out,
    vg_out,
    own,
    near,
    far,
    meta_mine,
    meta,
    bias,
    weight,
    outs,
    outs_other,
    own_terms,
    near_terms,
    other_send,
    other_got,
    far_send,
    far_got,
    near_send,
    near_got,
    result,
    load_sem,
    own_ssem,
    own_rsem,
    near_ssem,
    near_rsem,
    far_ssem,
    far_rsem,
    meta_ssem,
    meta_rsem,
    outs_ssem,
    outs_rsem,
    store_sem,
    other_ssem,
    other_rsem,
    fterm_ssem,
    fterm_rsem,
    nterm_ssem,
    nterm_rsem,
):
    D = HEAD_DIM
    me = lax.axis_index("seq")
    hd = lax.axis_index("head")
    chip, core = me // 2, lax.rem(me, 2)
    right, left = lax.rem(chip + 1, n_chip), lax.rem(chip + n_chip - 1, n_chip)
    ins = (q_in, k_in, v_in, g_in)

    def at_chip(offset):
        return lax.rem(chip + n_chip + offset, n_chip)

    def half(which):
        return pl.ds(pl.multiple_of(which * rows, rows), rows)

    def columns(which, h):
        return pl.ds(pl.multiple_of((which * heads + h) * D, D), D)

    def remote(src, dst, ssem, rsem, to_chip, to_core, to_hd=None):
        return pltpu.make_async_remote_copy(
            src_ref=src,
            dst_ref=dst,
            send_sem=ssem,
            recv_sem=rsem,
            device_id=(to_chip * 2 + to_core, hd if to_hd is None else to_hd),
            device_id_type=MESH,
        )

    def load(t, h):
        return pltpu.make_async_copy(
            ins[t].at[:, columns(core, h)], own.at[t, h, half(core)], load_sem.at[t, h]
        )

    for t in range(4):
        for h in range(heads):
            load(t, h).start()

    peers = []
    for offset in (-2, -1, 0, 1, 2):
        for c in range(2):
            for d in range(2):
                if offset == 0:
                    if c == 0 and d == 0:
                        continue
                    peers.append((0, lax.rem(core + c, 2), lax.rem(hd + d, 2)))
                else:
                    peers.append((offset, c, d))

    barrier = pltpu.get_barrier_semaphore()
    for offset, c, d in peers:
        pl.semaphore_signal(
            barrier, inc=1, device_id=(at_chip(offset) * 2 + c, d), device_id_type=MESH
        )

    packed = ids_in[...] * 2 + mask_in[...]
    wide = jnp.concatenate([packed, packed], axis=1)
    lane = lax.broadcasted_iota(jnp.int32, (1, 128), 1)
    wide = jnp.where((lane // 64) == hd, wide, 0)
    meta_mine[...] = wide
    meta[8 + core * 2 + hd] = wide

    pl.semaphore_wait(barrier, len(peers))

    def near_copy(h, c, t):
        return remote(
            ins[1 + t].at[:, columns(c, h)],
            near.at[t, h, half(core)],
            near_ssem.at[h, c, t],
            near_rsem.at[h, core, t],
            right,
            c,
        )

    def near_arrival(h, c, t):
        return remote(
            near.at[t, h, half(c)], near.at[t, h, half(c)], near_ssem.at[h, c, t], near_rsem.at[h, c, t], right, core
        )

    def far_copy(h, t):
        return remote(near.at[t, h], far.at[t, h], far_ssem.at[h, t], far_rsem.at[h, t], right, core)

    def send_near(h):
        for t in range(2):
            for c in range(2):
                near_copy(h, c, t).start()

    def relay(h):
        for c in range(2):
            for t in range(2):
                near_arrival(h, c, t).wait_recv()
        for t in range(2):
            far_copy(h, t).start()

    def own_copy(t, h):
        return remote(
            ins[t].at[:, columns(1 - core, h)],
            own.at[t, h, half(core)],
            own_ssem.at[t, h],
            own_rsem.at[t, h],
            chip,
            1 - core,
        )

    def meta_copy(peer):
        offset, c, d = peer
        return remote(
            meta_mine,
            meta.at[(2 - offset) * 4 + core * 2 + hd],
            meta_ssem.at[(2 + offset) * 4 + c * 2 + d],
            meta_rsem.at[(2 - offset) * 4 + core * 2 + hd],
            at_chip(offset),
            c,
            d,
        )

    def meta_arrival(peer):
        offset, c, d = peer
        place = (2 + offset) * 4 + c * 2 + d
        return remote(meta_mine, meta.at[place], meta_ssem.at[place], meta_rsem.at[place], at_chip(offset), c, d)

    send_near(0)
    for peer in peers:
        meta_copy(peer).start()
    for h in range(heads):
        for t in range(4):
            own_copy(t, h).start()
    send_near(1)

    relay(0)
    send_near(2)

    for peer in peers:
        meta_arrival(peer).wait_recv()

    def row_of(place):
        return meta[4 * (place // 2) + 2 * (place % 2)] + meta[4 * (place // 2) + 2 * (place % 2) + 1]

    key_rows = [row_of(place) for place in range(10)]
    key_docs = [r // 2 for r in key_rows]
    key_loss = [(r - 2 * (r // 2)).astype(jnp.float32) for r in key_rows]
    for part in range(2):
        mine = jnp.broadcast_to(key_rows[4 + part].astype(jnp.float32), (128, 128)).T.astype(jnp.int32)
        doc_q = mine // 2
        loss_q = (mine - 2 * doc_q).astype(jnp.float32)
        count = jnp.zeros((128, 128), jnp.float32)
        for place in range(10):
            same = doc_q == key_docs[place]
            count = count + jnp.where(same, key_loss[place], 0.0)
            if place < 6:
                if place == 4 + part:
                    q_at = lax.broadcasted_iota(jnp.int32, (128, 128), 0)
                    k_at = lax.broadcasted_iota(jnp.int32, (128, 128), 1)
                    same = jnp.logical_and(same, k_at <= q_at)
                if place > 4 + part:
                    block = jnp.full((128, 128), MASKED, jnp.float32)
                else:
                    block = jnp.where(same, 0.0, MASKED)
                bias[part * 128 : part * 128 + 128, place * 128 : place * 128 + 128] = block
        count = jnp.sum(count, axis=1, keepdims=True)
        weight[part * 128 : part * 128 + 128, :] = loss_q * float(rows) / jnp.maximum(count, float(rows // 8))

    for t in range(4):
        for h in range(heads):
            load(t, h).wait()
            remote(
                own.at[t, h, half(1 - core)],
                own.at[t, h, half(1 - core)],
                own_ssem.at[t, h],
                own_rsem.at[t, h],
                chip,
                1 - core,
            ).wait_recv()

    relay(1)
    send_near(3)

    def outs_copy(t, h):
        return remote(
            outs.at[t, h, half(1 - core)],
            outs_other.at[t, h],
            outs_ssem.at[t, h],
            outs_rsem.at[t, h],
            chip,
            1 - core,
        )

    def other_copy(t, h):
        return remote(
            other_send.at[t, h], other_got.at[t, h], other_ssem.at[t, h], other_rsem.at[t, h], chip, 1 - core
        )

    def fterm_copy(t, h):
        return remote(far_send.at[t, h], far_got.at[t, h], fterm_ssem.at[t, h], fterm_rsem.at[t, h], left, core)

    def nterm_copy(t, h, c):
        return remote(
            near_send.at[t, h, half(c)],
            near_got.at[t, core * heads + h],
            nterm_ssem.at[t, h, c],
            nterm_rsem.at[t, core * heads + h],
            left,
            c,
        )

    def store(t, h):
        return pltpu.make_async_copy(
            outs.at[t, h, half(core)], (o_out, qg_out)[t].at[:, columns(core, h)], store_sem.at[t, core * heads + h]
        )

    def store_other(t, h):
        return pltpu.make_async_copy(
            outs_other.at[t, h],
            (o_out, qg_out)[t].at[:, columns(1 - core, h)],
            store_sem.at[t, (1 - core) * heads + h],
        )

    def result_copy(t, j):
        return pltpu.make_async_copy(
            result.at[t, j], (kg_out, vg_out)[t].at[:, pl.ds(j * D, D)], store_sem.at[2 + t, j]
        )

    def send_nterm(h):
        for t in range(2):
            fterm_copy(t, h).wait_recv()
        for t in range(2):
            near_send[t, h] = (near_terms[t, h] + far_got[t, h].astype(jnp.float32)).astype(jnp.bfloat16)
        for t in range(2):
            for c in range(2):
                nterm_copy(t, h, c).start()

    def one_head(h, carry):
        for t in range(2):
            far_copy(h, t).wait_recv()
        q, g = own[0, h], (weight[...] * own[3, h].astype(jnp.float32)).astype(jnp.bfloat16)
        ks = (far[0, h], near[0, h], own[1, h])
        vs = (far[1, h], near[1, h], own[2, h])
        width = 2 * rows
        scores = [dot(q, ks[b], NT) * SCALE + bias[:, b * width : (b + 1) * width] for b in range(3)]
        top = jnp.max(functools.reduce(jnp.maximum, scores), axis=1, keepdims=True)
        prob = [jnp.exp(s - top) for s in scores]
        total = jnp.sum(prob[0] + prob[1] + prob[2], axis=1, keepdims=True)
        inverse = 1.0 / total
        prob = [p * inverse for p in prob]
        prob_half = [p.astype(jnp.bfloat16) for p in prob]
        attended = sum(dot(prob_half[b], vs[b], NN) for b in range(3)).astype(jnp.bfloat16)
        outs[0, h] = attended
        delta = jnp.sum(g.astype(jnp.float32) * attended.astype(jnp.float32), axis=1, keepdims=True)
        score_grad = [
            (prob[b] * (dot(g, vs[b], NT) - delta) * SCALE).astype(jnp.bfloat16) for b in range(3)
        ]
        far_send[0, h] = dot(score_grad[0], q, TN).astype(jnp.bfloat16)
        far_send[1, h] = dot(prob_half[0], g, TN).astype(jnp.bfloat16)
        outs[1, h] = sum(dot(score_grad[b], ks[b], NN) for b in range(3)).astype(jnp.bfloat16)
        near_terms[0, h] = dot(score_grad[1], q, TN)
        near_terms[1, h] = dot(prob_half[1], g, TN)
        own_terms[0, h] = dot(score_grad[2], q, TN)
        own_terms[1, h] = dot(prob_half[2], g, TN)
        for t in range(2):
            fterm_copy(t, h).start()
        for t in range(2):
            other_send[t, h] = own_terms[t, h, half(1 - core)].astype(jnp.bfloat16)

        @pl.when(h < heads - 2)
        def _():
            relay(h + 2)

        @pl.when(h > 0)
        def _():
            send_nterm(h - 1)

        for t in range(2):
            outs_copy(t, h).start()
            other_copy(t, h).start()
            store(t, h).start()
        return carry

    lax.fori_loop(0, heads, one_head, 0)
    send_nterm(heads - 1)

    for h in range(heads):
        for t in range(2):
            outs_copy(t, h).wait_recv()
            store_other(t, h).start()
            other_copy(t, h).wait_recv()

    for h in range(heads):
        for t in range(2):
            for c in range(2):
                j = c * heads + h
                remote(
                    near_send.at[t, h, half(c)],
                    near_got.at[t, j],
                    nterm_ssem.at[t, h, c],
                    nterm_rsem.at[t, j],
                    left,
                    core,
                ).wait_recv()
                mine = own_terms[t, h, half(core)]
                other = other_got[t, h].astype(jnp.float32)
                term = jnp.where(core == c, mine, other)
                result[t, j] = (term + near_got[t, j].astype(jnp.float32)).astype(jnp.bfloat16)
        for t in range(2):
            for c in range(2):
                result_copy(t, c * heads + h).start()

    for peer in peers:
        meta_copy(peer).wait_send()
    for h in range(heads):
        for t in range(4):
            own_copy(t, h).wait_send()
        for t in range(2):
            far_copy(h, t).wait_send()
            outs_copy(t, h).wait_send()
            other_copy(t, h).wait_send()
            fterm_copy(t, h).wait_send()
            store(t, h).wait()
            store_other(t, h).wait()
            for c in range(2):
                near_copy(h, c, t).wait_send()
                nterm_copy(t, h, c).wait_send()
                result_copy(t, c * heads + h).wait()


def solution(mesh):
    n_chip = mesh.shape["seq"] // 2

    def body(queries, keys, values, grad_out, doc_ids, loss_mask):
        rows, width = queries.shape
        heads = width // HEAD_DIM // 2
        D = HEAD_DIM
        bf16, f32 = jnp.bfloat16, jnp.float32
        dma = pltpu.SemaphoreType.DMA
        shape = jax.ShapeDtypeStruct((rows, width), bf16)
        vmem = pltpu.VMEM
        return pl.pallas_call(
            functools.partial(kernel, n_chip, rows, heads),
            out_shape=(shape,) * 4,
            in_specs=[pl.BlockSpec(memory_space=pl.ANY)] * 4 + [pl.BlockSpec(memory_space=pltpu.VMEM)] * 2,
            out_specs=(pl.BlockSpec(memory_space=pl.ANY),) * 4,
            scratch_shapes=[
                vmem((4, heads, 2 * rows, D), bf16),
                vmem((2, heads, 2 * rows, D), bf16),
                vmem((2, heads, 2 * rows, D), bf16),
                vmem((1, 128), jnp.int32),
                vmem((20, 1, 128), jnp.int32),
                vmem((2 * rows, 6 * rows), f32),
                vmem((2 * rows, 128), f32),
                vmem((2, heads, 2 * rows, D), bf16),
                vmem((2, heads, rows, D), bf16),
                vmem((2, heads, 2 * rows, D), f32),
                vmem((2, heads, 2 * rows, D), f32),
                vmem((2, heads, rows, D), bf16),
                vmem((2, heads, rows, D), bf16),
                vmem((2, heads, 2 * rows, D), bf16),
                vmem((2, heads, 2 * rows, D), bf16),
                vmem((2, heads, 2 * rows, D), bf16),
                vmem((2, 2 * heads, rows, D), bf16),
                vmem((2, 2 * heads, rows, D), bf16),
                dma((4, heads)),
                dma((4, heads)),
                dma((4, heads)),
                dma((heads, 2, 2)),
                dma((heads, 2, 2)),
                dma((heads, 2)),
                dma((heads, 2)),
                dma((20,)),
                dma((20,)),
                dma((2, heads)),
                dma((2, heads)),
                dma((4, 2 * heads)),
                dma((2, heads)),
                dma((2, heads)),
                dma((2, heads)),
                dma((2, heads)),
                dma((2, heads, 2)),
                dma((2, 2 * heads)),
            ],
            compiler_params=pltpu.CompilerParams(
                collective_id=0, has_side_effects=True, vmem_limit_bytes=60 * 1024 * 1024
            ),
        )(queries, keys, values, grad_out, doc_ids.reshape(1, -1), loss_mask.reshape(1, -1))

    return jax.shard_map(
        body,
        mesh=mesh,
        in_specs=(P("seq", "head"),) * 4 + (P(("seq", "head")),) * 2,
        out_specs=(P("seq", "head"),) * 4,
        check_vma=False,
    )
```

```python
import functools
import math

import jax
import jax.numpy as jnp
from jax import lax
from jax.experimental import pallas as pl
from jax.experimental.pallas import tpu as pltpu
from jax.sharding import PartitionSpec as P

HEAD_DIM = 128
MASKED = -1e30
SCALE = 1.0 / math.sqrt(HEAD_DIM)
MESH = pl.DeviceIdType.MESH
NN = (((1,), (0,)), ((), ()))
NT = (((1,), (1,)), ((), ()))
TN = (((0,), (0,)), ((), ()))


def dot(a, b, dims):
    return lax.dot_general(a, b, dims, preferred_element_type=jnp.float32)


def kernel(
    n_chip,
    rows,
    heads,
    q_in,
    k_in,
    v_in,
    g_in,
    ids_in,
    mask_in,
    o_out,
    qg_out,
    kg_out,
    vg_out,
    kv_mine,
    ids_mask,
    own,
    near,
    far,
    meta_mine,
    meta,
    bias,
    weight,
    outs,
    outs_other,
    own_terms,
    near_terms,
    other_send,
    other_got,
    far_send,
    far_got,
    near_send,
    near_got,
    load_sem,
    kv_sem,
    ids_sem,
    own_ssem,
    own_rsem,
    near_ssem,
    near_rsem,
    far_ssem,
    far_rsem,
    meta_ssem,
    meta_rsem,
    outs_ssem,
    outs_rsem,
    other_ssem,
    other_rsem,
    fterm_ssem,
    fterm_rsem,
    nterm_ssem,
    nterm_rsem,
):
    D = HEAD_DIM
    me = lax.axis_index("seq")
    hd = lax.axis_index("head")
    chip, core = me // 2, lax.rem(me, 2)
    right, left = lax.rem(chip + 1, n_chip), lax.rem(chip + n_chip - 1, n_chip)
    ins = (q_in, k_in, v_in, g_in)

    has_left, has_left2 = chip >= 1, chip >= 2
    has_right, has_right2 = chip <= n_chip - 2, chip <= n_chip - 3
    exists = {-2: has_left2, -1: has_left, 1: has_right, 2: has_right2}

    def at_chip(offset):
        return lax.rem(chip + n_chip + offset, n_chip)

    def where_chip(offset, act):
        if offset == 0:
            act()
        else:
            pl.when(exists[offset])(act)

    def half(which):
        return pl.ds(pl.multiple_of(which * rows, rows), rows)

    def columns(which, h):
        return pl.ds(pl.multiple_of((which * heads + h) * D, D), D)

    def remote(src, dst, ssem, rsem, to_chip, to_core, to_hd=None):
        return pltpu.make_async_remote_copy(
            src_ref=src,
            dst_ref=dst,
            send_sem=ssem,
            recv_sem=rsem,
            device_id=(to_chip * 2 + to_core, hd if to_hd is None else to_hd),
            device_id_type=MESH,
        )

    peers = []
    for offset in (-2, -1, 0, 1, 2):
        for c in range(2):
            for d in range(2):
                if offset == 0:
                    if c == 0 and d == 0:
                        continue
                    peers.append((0, lax.rem(core + c, 2), lax.rem(hd + d, 2)))
                else:
                    peers.append((offset, c, d))

    def peers_at(offset):
        return [peer for peer in peers if peer[0] == offset]

    barrier = pltpu.get_barrier_semaphore()
    for offset in (-2, -1, 0, 1, 2):

        @functools.partial(where_chip, offset)
        def _(offset=offset):
            for _, c, d in peers_at(offset):
                pl.semaphore_signal(
                    barrier, inc=1, device_id=(at_chip(offset) * 2 + c, d), device_id_type=MESH
                )

    def kv_load(t):
        return pltpu.make_async_copy(ins[1 + t], kv_mine.at[t], kv_sem.at[t])

    def ids_load(t):
        return pltpu.make_async_copy((ids_in, mask_in)[t], ids_mask.at[t], ids_sem.at[t])

    for t in range(2):
        ids_load(t).start()
        kv_load(t).start()

    def load(t, h):
        return pltpu.make_async_copy(
            ins[t].at[:, columns(core, h)], own.at[t, h, half(core)], load_sem.at[t, h]
        )

    for t in range(4):
        for h in range(heads):
            load(t, h).start()

    @pl.when(jnp.logical_not(has_left))
    def _():
        near[...] = jnp.zeros_like(near)

    @pl.when(jnp.logical_not(has_left2))
    def _():
        far[...] = jnp.zeros_like(far)

    @pl.when(jnp.logical_not(has_right))
    def _():
        near_got[...] = jnp.zeros_like(near_got)

    @pl.when(jnp.logical_not(jnp.logical_and(has_left, has_right)))
    def _():
        far_got[...] = jnp.zeros_like(far_got)

    for offset in (-2, -1, 1, 2):

        @pl.when(jnp.logical_not(exists[offset]))
        def _(offset=offset):
            for c in range(2):
                meta[(2 + offset) * 4 + c * 2] = jnp.full((1, 128), -2, jnp.int32)
                meta[(2 + offset) * 4 + c * 2 + 1] = jnp.zeros((1, 128), jnp.int32)

    for t in range(2):
        ids_load(t).wait()
    packed = ids_mask[0] * 2 + ids_mask[1]
    wide = jnp.concatenate([packed, packed], axis=1)
    lane = lax.broadcasted_iota(jnp.int32, (1, 128), 1)
    wide = jnp.where((lane // 64) == hd, wide, 0)
    meta_mine[...] = wide
    meta[8 + core * 2 + hd] = wide

    for t in range(2):
        kv_load(t).wait()
    there = sum(exists[offset].astype(jnp.int32) for offset in (-2, -1, 1, 2))
    pl.semaphore_wait(barrier, 3 + 4 * there)

    def near_copy(h, c, t):
        return remote(
            kv_mine.at[t, :, columns(c, h)],
            near.at[t, h, half(core)],
            near_ssem.at[h, c, t],
            near_rsem.at[h, core, t],
            right,
            c,
        )

    def near_arrival(h, c, t):
        return remote(
            near.at[t, h, half(c)], near.at[t, h, half(c)], near_ssem.at[h, c, t], near_rsem.at[h, c, t], right, core
        )

    def far_copy(h, c, t):
        return remote(
            near.at[t, h, half(c)],
            far.at[t, h, half(c)],
            far_ssem.at[h, c, t],
            far_rsem.at[h, c, t],
            right,
            core,
        )

    def send_near(h):
        @pl.when(has_right)
        def _():
            for t in range(2):
                for c in range(2):
                    near_copy(h, c, t).start()

    def relay(h):
        @pl.when(has_left)
        def _():
            for t in range(2):
                for c in range(2):
                    near_arrival(h, c, t).wait_recv()

                    @pl.when(has_right)
                    def _():
                        far_copy(h, c, t).start()

    def own_copy(t, h):
        return remote(
            ins[t].at[:, columns(1 - core, h)],
            own.at[t, h, half(core)],
            own_ssem.at[t, h],
            own_rsem.at[t, h],
            chip,
            1 - core,
        )

    def meta_copy(peer):
        offset, c, d = peer
        return remote(
            meta_mine,
            meta.at[(2 - offset) * 4 + core * 2 + hd],
            meta_ssem.at[(2 + offset) * 4 + c * 2 + d],
            meta_rsem.at[(2 - offset) * 4 + core * 2 + hd],
            at_chip(offset),
            c,
            d,
        )

    def meta_arrival(peer):
        offset, c, d = peer
        place = (2 + offset) * 4 + c * 2 + d
        return remote(meta_mine, meta.at[place], meta_ssem.at[place], meta_rsem.at[place], at_chip(offset), c, d)

    for offset in (0, -1, 1, -2, 2):

        @functools.partial(where_chip, offset)
        def _(offset=offset):
            for peer in peers_at(offset):
                meta_copy(peer).start()

    for h in range(heads):
        send_near(h)
        for t in range(4):
            own_copy(t, h).start()
    for h in range(heads):
        relay(h)

    for offset in (0, -1, 1, -2, 2):

        @functools.partial(where_chip, offset)
        def _(offset=offset):
            for peer in peers_at(offset):
                meta_arrival(peer).wait_recv()

    def row_of(place):
        return meta[4 * (place // 2) + 2 * (place % 2)] + meta[4 * (place // 2) + 2 * (place % 2) + 1]

    key_rows = [row_of(place) for place in range(10)]
    key_docs = [r // 2 for r in key_rows]
    key_loss = [(r - 2 * (r // 2)).astype(jnp.float32) for r in key_rows]
    for part in range(2):
        mine = jnp.broadcast_to(key_rows[4 + part].astype(jnp.float32), (128, 128)).T.astype(jnp.int32)
        doc_q = mine // 2
        loss_q = (mine - 2 * doc_q).astype(jnp.float32)
        count = jnp.zeros((128, 128), jnp.float32)
        for place in range(10):
            same = doc_q == key_docs[place]
            count = count + jnp.where(same, key_loss[place], 0.0)
            if place < 6:
                if place == 4 + part:
                    q_at = lax.broadcasted_iota(jnp.int32, (128, 128), 0)
                    k_at = lax.broadcasted_iota(jnp.int32, (128, 128), 1)
                    same = jnp.logical_and(same, k_at <= q_at)
                if place > 4 + part:
                    block = jnp.full((128, 128), MASKED, jnp.float32)
                else:
                    block = jnp.where(same, 0.0, MASKED)
                bias[part * 128 : part * 128 + 128, place * 128 : place * 128 + 128] = block
        count = jnp.sum(count, axis=1, keepdims=True)
        weight[part * 128 : part * 128 + 128, :] = loss_q * float(rows) / jnp.maximum(count, float(rows // 8))

    for t in range(4):
        for h in range(heads):
            load(t, h).wait()
            remote(
                own.at[t, h, half(1 - core)],
                own.at[t, h, half(1 - core)],
                own_ssem.at[t, h],
                own_rsem.at[t, h],
                chip,
                1 - core,
            ).wait_recv()

    def outs_copy(t, h):
        return remote(
            outs.at[t, h, half(1 - core)],
            outs_other.at[t, h],
            outs_ssem.at[t, h],
            outs_rsem.at[t, h],
            chip,
            1 - core,
        )

    def other_copy(t, h):
        return remote(
            other_send.at[t, h], other_got.at[t, h], other_ssem.at[t, h], other_rsem.at[t, h], chip, 1 - core
        )

    def fterm_copy(t, h):
        return remote(far_send.at[t, h], far_got.at[t, h], fterm_ssem.at[t, h], fterm_rsem.at[t, h], left, core)

    def nterm_copy(t, h, c):
        return remote(
            near_send.at[t, h, half(c)],
            near_got.at[t, core * heads + h],
            nterm_ssem.at[t, h, c],
            nterm_rsem.at[t, core * heads + h],
            left,
            c,
        )

    def send_nterm(h):
        @pl.when(jnp.logical_and(has_left, has_right))
        def _():
            for t in range(2):
                fterm_copy(t, h).wait_recv()

        @pl.when(has_left)
        def _():
            for t in range(2):
                near_send[t, h] = (near_terms[t, h] + far_got[t, h].astype(jnp.float32)).astype(jnp.bfloat16)
            for t in range(2):
                for c in range(2):
                    nterm_copy(t, h, c).start()

    def one_head(h, carry):
        @pl.when(has_left2)
        def _():
            for t in range(2):
                for c in range(2):
                    far_copy(h, c, t).wait_recv()


        @pl.when(jnp.logical_and(h == 3, jnp.logical_and(has_left2, lax.rem(chip, 4) == 0)))
        def _():
            for i in (0, 1, 2):
                for t in range(2):
                    fterm_copy(t, i).start()


        @pl.when(jnp.logical_and(h == 3, jnp.logical_and(has_left2, lax.rem(chip, 4) != 0)))
        def _():
            for i in (0, 1):
                for t in range(2):
                    fterm_copy(t, i).start()

        q, g = own[0, h], (weight[...] * own[3, h].astype(jnp.float32)).astype(jnp.bfloat16)
        ks = (far[0, h], near[0, h], own[1, h])
        vs = (far[1, h], near[1, h], own[2, h])
        width = 2 * rows
        scores = [dot(q, ks[b], NT) * SCALE + bias[:, b * width : (b + 1) * width] for b in range(3)]
        top = jnp.max(functools.reduce(jnp.maximum, scores), axis=1, keepdims=True)
        prob = [jnp.exp(s - top) for s in scores]
        total = jnp.sum(prob[0] + prob[1] + prob[2], axis=1, keepdims=True)
        inverse = 1.0 / total
        prob = [p * inverse for p in prob]
        prob_half = [p.astype(jnp.bfloat16) for p in prob]
        attended = sum(dot(prob_half[b], vs[b], NN) for b in range(3)).astype(jnp.bfloat16)
        outs[0, h] = attended
        delta = jnp.sum(g.astype(jnp.float32) * attended.astype(jnp.float32), axis=1, keepdims=True)
        score_grad = [
            (prob[b] * (dot(g, vs[b], NT) - delta) * SCALE).astype(jnp.bfloat16) for b in range(3)
        ]
        far_send[0, h] = dot(score_grad[0], q, TN).astype(jnp.bfloat16)
        far_send[1, h] = dot(prob_half[0], g, TN).astype(jnp.bfloat16)
        outs[1, h] = sum(dot(score_grad[b], ks[b], NN) for b in range(3)).astype(jnp.bfloat16)
        near_terms[0, h] = dot(score_grad[1], q, TN)
        near_terms[1, h] = dot(prob_half[1], g, TN)
        own_terms[0, h] = dot(score_grad[2], q, TN)
        own_terms[1, h] = dot(prob_half[2], g, TN)
        for t in range(2):
            other_send[t, h] = own_terms[t, h, half(1 - core)].astype(jnp.bfloat16)

        for t in range(2):
            outs_copy(t, h).start()
            other_copy(t, h).start()
            (o_out, qg_out)[t][:, columns(core, h)] = outs[t, h, half(core)]
        return carry

    lax.fori_loop(0, heads, one_head, 0)
    @pl.when(jnp.logical_and(has_left2, lax.rem(chip, 4) == 0))
    def _():
        for i in (3,):
            for t in range(2):
                fterm_copy(t, i).start()

    @pl.when(jnp.logical_and(has_left2, lax.rem(chip, 4) != 0))
    def _():
        for i in (2, 3):
            for t in range(2):
                fterm_copy(t, i).start()

    for h in range(heads):
        send_nterm(h)

    for h in range(heads):
        for t in range(2):
            outs_copy(t, h).wait_recv()
            (o_out, qg_out)[t][:, columns(1 - core, h)] = outs_other[t, h]
            other_copy(t, h).wait_recv()

    for h in range(heads):
        for t in range(2):
            for c in range(2):
                j = c * heads + h

                @pl.when(has_right)
                def _():
                    remote(
                        near_send.at[t, h, half(c)],
                        near_got.at[t, j],
                        nterm_ssem.at[t, h, c],
                        nterm_rsem.at[t, j],
                        left,
                        core,
                    ).wait_recv()

                mine = own_terms[t, h, half(core)]
                other = other_got[t, h].astype(jnp.float32)
                term = jnp.where(core == c, mine, other)
                (kg_out, vg_out)[t][:, j * D : (j + 1) * D] = (
                    term + near_got[t, j].astype(jnp.float32)
                ).astype(jnp.bfloat16)

    for offset in (-2, -1, 0, 1, 2):

        @functools.partial(where_chip, offset)
        def _(offset=offset):
            for peer in peers_at(offset):
                meta_copy(peer).wait_send()

    for h in range(heads):
        for t in range(4):
            own_copy(t, h).wait_send()
        for t in range(2):
            outs_copy(t, h).wait_send()
            other_copy(t, h).wait_send()

    @pl.when(has_right)
    def _():
        for h in range(heads):
            for t in range(2):
                for c in range(2):
                    near_copy(h, c, t).wait_send()

    @pl.when(jnp.logical_and(has_left, has_right))
    def _():
        for h in range(heads):
            for t in range(2):
                for c in range(2):
                    far_copy(h, c, t).wait_send()

    @pl.when(has_left2)
    def _():
        for h in range(heads):
            for t in range(2):
                fterm_copy(t, h).wait_send()

    @pl.when(has_left)
    def _():
        for h in range(heads):
            for t in range(2):
                for c in range(2):
                    nterm_copy(t, h, c).wait_send()


def write_kernel(*refs):
    sems = refs[-1]
    n = (len(refs) - 1) // 2
    copies = [pltpu.make_async_copy(refs[i], refs[n + i], sems.at[i]) for i in range(n)]
    for copy in copies:
        copy.start()
    for copy in copies:
        copy.wait()


def solution(mesh):
    n_chip = mesh.shape["seq"] // 2

    def body(queries, keys, values, grad_out, doc_ids, loss_mask):
        rows, width = queries.shape
        heads = width // HEAD_DIM // 2
        D = HEAD_DIM
        bf16, f32 = jnp.bfloat16, jnp.float32
        dma = pltpu.SemaphoreType.DMA
        shape = jax.ShapeDtypeStruct((rows, width), bf16)
        vmem = pltpu.VMEM
        held = pl.pallas_call(
            functools.partial(kernel, n_chip, rows, heads),
            out_shape=(pltpu.VMEM((rows, width), bf16),) * 4,
            in_specs=[pl.BlockSpec(memory_space=pl.ANY)] * 6,
            out_specs=(pl.BlockSpec(memory_space=pltpu.VMEM),) * 4,
            scratch_shapes=[
                vmem((2, rows, width), bf16),
                vmem((2, 1, 64), jnp.int32),
                vmem((4, heads, 2 * rows, D), bf16),
                vmem((2, heads, 2 * rows, D), bf16),
                vmem((2, heads, 2 * rows, D), bf16),
                vmem((1, 128), jnp.int32),
                vmem((20, 1, 128), jnp.int32),
                vmem((2 * rows, 6 * rows), f32),
                vmem((2 * rows, 128), f32),
                vmem((2, heads, 2 * rows, D), bf16),
                vmem((2, heads, rows, D), bf16),
                vmem((2, heads, 2 * rows, D), f32),
                vmem((2, heads, 2 * rows, D), f32),
                vmem((2, heads, rows, D), bf16),
                vmem((2, heads, rows, D), bf16),
                vmem((2, heads, 2 * rows, D), bf16),
                vmem((2, heads, 2 * rows, D), bf16),
                vmem((2, heads, 2 * rows, D), bf16),
                vmem((2, 2 * heads, rows, D), bf16),
                dma((4, heads)),
                dma((2,)),
                dma((2,)),
                dma((4, heads)),
                dma((4, heads)),
                dma((heads, 2, 2)),
                dma((heads, 2, 2)),
                dma((heads, 2, 2)),
                dma((heads, 2, 2)),
                dma((20,)),
                dma((20,)),
                dma((2, heads)),
                dma((2, heads)),
                dma((2, heads)),
                dma((2, heads)),
                dma((2, heads)),
                dma((2, heads)),
                dma((2, heads, 2)),
                dma((2, 2 * heads)),
            ],
            compiler_params=pltpu.CompilerParams(
                collective_id=0, has_side_effects=True, vmem_limit_bytes=60 * 1024 * 1024
            ),
        )(queries, keys, values, grad_out, doc_ids.reshape(1, -1), loss_mask.reshape(1, -1))
        return pl.pallas_call(
            write_kernel,
            out_shape=(shape,) * 4,
            in_specs=[pl.BlockSpec(memory_space=pltpu.VMEM)] * 4,
            out_specs=(pl.BlockSpec(memory_space=pl.ANY),) * 4,
            scratch_shapes=[dma((4,))],
        )(*(pltpu.with_memory_space_constraint(x, pltpu.VMEM) for x in held))

    return jax.shard_map(
        body,
        mesh=mesh,
        in_specs=(P("seq", "head"),) * 4 + (P(("seq", "head")),) * 2,
        out_specs=(P("seq", "head"),) * 4,
        check_vma=False,
    )
```

```python
import functools
import math

import jax
import jax.numpy as jnp
from jax import lax
from jax.experimental import pallas as pl
from jax.experimental.pallas import tpu as pltpu
from jax.sharding import PartitionSpec as P

HEAD_DIM = 128
MASKED = -1e30
SCALE = 1.0 / math.sqrt(HEAD_DIM)
MESH = pl.DeviceIdType.MESH
NN = (((1,), (0,)), ((), ()))
NT = (((1,), (1,)), ((), ()))
TN = (((0,), (0,)), ((), ()))


def dot(a, b, dims):
    return lax.dot_general(a, b, dims, preferred_element_type=jnp.float32)


def kernel(
    n_chip,
    rows,
    heads,
    q_in,
    k_in,
    v_in,
    g_in,
    ids_in,
    mask_in,
    o_out,
    qg_out,
    kg_out,
    vg_out,
    kv_mine,
    ids_mask,
    own,
    near,
    far,
    meta,
    bias,
    weight,
    outs,
    outs_other,
    own_terms,
    near_terms,
    other_send,
    other_got,
    far_send,
    far_got,
    near_send,
    near_got,
    load_sem,
    kv_sem,
    ids_sem,
    own_ssem,
    own_rsem,
    near_ssem,
    near_rsem,
    far_ssem,
    far_rsem,
    half_ssem,
    half_rsem,
    rows_ssem,
    rows_rsem,
    past_ssem,
    past_rsem,
    outs_ssem,
    outs_rsem,
    other_ssem,
    other_rsem,
    fterm_ssem,
    fterm_rsem,
    nterm_ssem,
    nterm_rsem,
):
    D = HEAD_DIM
    me = lax.axis_index("seq")
    hd = lax.axis_index("head")
    chip, core = me // 2, lax.rem(me, 2)
    right, left = lax.rem(chip + 1, n_chip), lax.rem(chip + n_chip - 1, n_chip)
    ins = (q_in, k_in, v_in, g_in)

    has_left, has_left2 = chip >= 1, chip >= 2
    has_right, has_right2 = chip <= n_chip - 2, chip <= n_chip - 3
    exists = {-2: has_left2, -1: has_left, 1: has_right, 2: has_right2}

    def at_chip(offset):
        return lax.rem(chip + n_chip + offset, n_chip)

    def where_chip(offset, act):
        if offset == 0:
            act()
        else:
            pl.when(exists[offset])(act)

    def half(which):
        return pl.ds(pl.multiple_of(which * rows, rows), rows)

    def columns(which, h):
        return pl.ds(pl.multiple_of((which * heads + h) * D, D), D)

    def remote(src, dst, ssem, rsem, to_chip, to_core, to_hd=None):
        return pltpu.make_async_remote_copy(
            src_ref=src,
            dst_ref=dst,
            send_sem=ssem,
            recv_sem=rsem,
            device_id=(to_chip * 2 + to_core, hd if to_hd is None else to_hd),
            device_id_type=MESH,
        )

    barrier = pltpu.get_barrier_semaphore()

    def greet(to_chip, to_core, to_hd):
        pl.semaphore_signal(barrier, inc=1, device_id=(to_chip * 2 + to_core, to_hd), device_id_type=MESH)

    for offset in (-1, 1):

        @functools.partial(where_chip, offset)
        def _(offset=offset):
            for c in range(2):
                greet(at_chip(offset), c, hd)

    greet(chip, 1 - core, hd)
    greet(chip, core, 1 - hd)

    def kv_load(t):
        return pltpu.make_async_copy(ins[1 + t], kv_mine.at[t], kv_sem.at[t])

    def ids_load(t):
        return pltpu.make_async_copy((ids_in, mask_in)[t], ids_mask.at[t], ids_sem.at[t])

    for t in range(2):
        ids_load(t).start()
        kv_load(t).start()

    def load(t, h):
        return pltpu.make_async_copy(
            ins[t].at[:, columns(core, h)], own.at[t, h, half(core)], load_sem.at[t, h]
        )

    for t in range(4):
        for h in range(heads):
            load(t, h).start()

    @pl.when(jnp.logical_not(has_left))
    def _():
        near[...] = jnp.zeros_like(near)

    @pl.when(jnp.logical_not(has_left2))
    def _():
        far[...] = jnp.zeros_like(far)

    @pl.when(jnp.logical_not(has_right))
    def _():
        near_got[...] = jnp.zeros_like(near_got)

    @pl.when(jnp.logical_not(jnp.logical_and(has_left, has_right)))
    def _():
        far_got[...] = jnp.zeros_like(far_got)

    for offset in (-2, -1, 1, 2):

        @pl.when(jnp.logical_not(exists[offset]))
        def _(offset=offset):
            for c in range(2):
                meta[(2 + offset) * 4 + c * 2] = jnp.full((1, 128), -2, jnp.int32)
                meta[(2 + offset) * 4 + c * 2 + 1] = jnp.zeros((1, 128), jnp.int32)

    for t in range(2):
        ids_load(t).wait()
    packed = ids_mask[0] * 2 + ids_mask[1]
    wide = jnp.concatenate([packed, packed], axis=1)
    lane = lax.broadcasted_iota(jnp.int32, (1, 128), 1)
    wide = jnp.where((lane // 64) == hd, wide, 0)
    meta[8 + core * 2 + hd] = wide

    for t in range(2):
        kv_load(t).wait()
    there = exists[-1].astype(jnp.int32) + exists[1].astype(jnp.int32)
    pl.semaphore_wait(barrier, 2 + 2 * there)

    def near_copy(h, c, t):
        return remote(
            kv_mine.at[t, :, columns(c, h)],
            near.at[t, h, half(core)],
            near_ssem.at[h, c, t],
            near_rsem.at[h, core, t],
            right,
            c,
        )

    def near_arrival(h, c, t):
        return remote(
            near.at[t, h, half(c)], near.at[t, h, half(c)], near_ssem.at[h, c, t], near_rsem.at[h, c, t], right, core
        )

    def far_copy(h, c, t):
        return remote(
            near.at[t, h, half(c)],
            far.at[t, h, half(c)],
            far_ssem.at[h, c, t],
            far_rsem.at[h, c, t],
            right,
            core,
        )

    def send_near(h):
        @pl.when(has_right)
        def _():
            for t in range(2):
                for c in range(2):
                    near_copy(h, c, t).start()

    def relay(h):
        @pl.when(has_left)
        def _():
            for t in range(2):
                for c in range(2):
                    near_arrival(h, c, t).wait_recv()

                    @pl.when(has_right)
                    def _():
                        far_copy(h, c, t).start()

    def own_copy(t, h):
        return remote(
            ins[t].at[:, columns(1 - core, h)],
            own.at[t, h, half(core)],
            own_ssem.at[t, h],
            own_rsem.at[t, h],
            chip,
            1 - core,
        )

    def half_copy():
        mine = meta.at[8 + core * 2 + hd]
        return remote(mine, mine, half_ssem.at[0], half_rsem.at[0], chip, core, 1 - hd)

    def rows_copy(offset, c):
        return remote(
            meta.at[pl.ds(8 + core * 2, 2)],
            meta.at[pl.ds((2 - offset) * 4 + core * 2, 2)],
            rows_ssem.at[1 + offset, c],
            rows_rsem.at[1 - offset, core],
            at_chip(offset),
            c,
        )

    def rows_arrival(offset, c):
        rows_there = meta.at[pl.ds((2 + offset) * 4 + c * 2, 2)]
        return remote(rows_there, rows_there, rows_ssem.at[1 + offset, c], rows_rsem.at[1 + offset, c], chip, 1 - core)

    def past_copy(offset):
        return remote(
            meta.at[pl.ds((2 - offset) * 4, 4)],
            meta.at[pl.ds((2 - 2 * offset) * 4, 4)],
            past_ssem.at[(1 - offset) // 2],
            past_rsem.at[(1 - offset) // 2],
            at_chip(offset),
            core,
        )

    def rows_to(offset, act):
        if offset == 0:
            act(0, 1 - core)
        else:

            @pl.when(exists[offset])
            def _():
                for c in range(2):
                    act(offset, c)

    inner = jnp.logical_and(has_left, has_right)

    half_copy().start()
    send_near(0)
    send_near(1)
    half_copy().wait_recv()
    for offset in (0, 1, -1):
        rows_to(offset, lambda offset, c: rows_copy(offset, c).start())
    for h in range(heads):
        for t in range(4):
            own_copy(t, h).start()
    send_near(2)
    relay(0)
    for offset in (0, 1, -1):
        rows_to(offset, lambda offset, c: rows_arrival(offset, c).wait_recv())

    @pl.when(inner)
    def _():
        past_copy(1).start()
        past_copy(-1).start()

    send_near(3)
    for h in range(1, heads):
        relay(h)

    @pl.when(has_left2)
    def _():
        past_copy(1).wait_recv()

    @pl.when(has_right2)
    def _():
        past_copy(-1).wait_recv()

    def row_of(place):
        return meta[4 * (place // 2) + 2 * (place % 2)] + meta[4 * (place // 2) + 2 * (place % 2) + 1]

    key_rows = [row_of(place) for place in range(10)]
    key_docs = [r // 2 for r in key_rows]
    key_loss = [(r - 2 * (r // 2)).astype(jnp.float32) for r in key_rows]
    for part in range(2):
        mine = jnp.broadcast_to(key_rows[4 + part].astype(jnp.float32), (128, 128)).T.astype(jnp.int32)
        doc_q = mine // 2
        loss_q = (mine - 2 * doc_q).astype(jnp.float32)
        count = jnp.zeros((128, 128), jnp.float32)
        for place in range(10):
            same = doc_q == key_docs[place]
            count = count + jnp.where(same, key_loss[place], 0.0)
            if place < 6:
                if place == 4 + part:
                    q_at = lax.broadcasted_iota(jnp.int32, (128, 128), 0)
                    k_at = lax.broadcasted_iota(jnp.int32, (128, 128), 1)
                    same = jnp.logical_and(same, k_at <= q_at)
                if place > 4 + part:
                    block = jnp.full((128, 128), MASKED, jnp.float32)
                else:
                    block = jnp.where(same, 0.0, MASKED)
                bias[part * 128 : part * 128 + 128, place * 128 : place * 128 + 128] = block
        count = jnp.sum(count, axis=1, keepdims=True)
        weight[part * 128 : part * 128 + 128, :] = loss_q * float(rows) / jnp.maximum(count, float(rows // 8))

    for t in range(4):
        for h in range(heads):
            load(t, h).wait()
            remote(
                own.at[t, h, half(1 - core)],
                own.at[t, h, half(1 - core)],
                own_ssem.at[t, h],
                own_rsem.at[t, h],
                chip,
                1 - core,
            ).wait_recv()

    def outs_copy(t, h):
        return remote(
            outs.at[t, h, half(1 - core)],
            outs_other.at[t, h],
            outs_ssem.at[t, h],
            outs_rsem.at[t, h],
            chip,
            1 - core,
        )

    def other_copy(t, h):
        return remote(
            other_send.at[t, h], other_got.at[t, h], other_ssem.at[t, h], other_rsem.at[t, h], chip, 1 - core
        )

    def fterm_copy(t, h):
        return remote(far_send.at[t, h], far_got.at[t, h], fterm_ssem.at[t, h], fterm_rsem.at[t, h], left, core)

    def nterm_copy(t, h, c):
        return remote(
            near_send.at[t, h, half(c)],
            near_got.at[t, core * heads + h],
            nterm_ssem.at[t, h, c],
            nterm_rsem.at[t, core * heads + h],
            left,
            c,
        )

    def send_nterm(h):
        @pl.when(jnp.logical_and(has_left, has_right))
        def _():
            for t in range(2):
                fterm_copy(t, h).wait_recv()

        @pl.when(has_left)
        def _():
            for t in range(2):
                near_send[t, h] = (near_terms[t, h] + far_got[t, h].astype(jnp.float32)).astype(jnp.bfloat16)
            for t in range(2):
                for c in range(2):
                    nterm_copy(t, h, c).start()

    def one_head(h, carry):
        @pl.when(has_left2)
        def _():
            for t in range(2):
                for c in range(2):
                    far_copy(h, c, t).wait_recv()

        @pl.when(jnp.logical_and(h == 2, jnp.logical_and(has_left2, lax.rem(chip, 4) == 0)))
        def _():
            for i in (0, 1):
                for t in range(2):
                    fterm_copy(t, i).start()

        q, g = own[0, h], (weight[...] * own[3, h].astype(jnp.float32)).astype(jnp.bfloat16)
        ks = (far[0, h], near[0, h], own[1, h])
        vs = (far[1, h], near[1, h], own[2, h])
        width = 2 * rows
        scores = [dot(q, ks[b], NT) * SCALE + bias[:, b * width : (b + 1) * width] for b in range(3)]
        top = jnp.max(functools.reduce(jnp.maximum, scores), axis=1, keepdims=True)
        prob = [jnp.exp(s - top) for s in scores]
        total = jnp.sum(prob[0] + prob[1] + prob[2], axis=1, keepdims=True)
        inverse = 1.0 / total
        prob = [p * inverse for p in prob]
        prob_half = [p.astype(jnp.bfloat16) for p in prob]
        attended = sum(dot(prob_half[b], vs[b], NN) for b in range(3)).astype(jnp.bfloat16)
        outs[0, h] = attended
        delta = jnp.sum(g.astype(jnp.float32) * attended.astype(jnp.float32), axis=1, keepdims=True)
        score_grad = [
            (prob[b] * (dot(g, vs[b], NT) - delta) * SCALE).astype(jnp.bfloat16) for b in range(3)
        ]
        far_send[0, h] = dot(score_grad[0], q, TN).astype(jnp.bfloat16)
        far_send[1, h] = dot(prob_half[0], g, TN).astype(jnp.bfloat16)
        outs[1, h] = sum(dot(score_grad[b], ks[b], NN) for b in range(3)).astype(jnp.bfloat16)
        near_terms[0, h] = dot(score_grad[1], q, TN)
        near_terms[1, h] = dot(prob_half[1], g, TN)
        own_terms[0, h] = dot(score_grad[2], q, TN)
        own_terms[1, h] = dot(prob_half[2], g, TN)

        @pl.when(jnp.logical_and(h == 2, jnp.logical_and(has_left2, lax.rem(chip, 4) == 0)))
        def _():
            for i in (2,):
                for t in range(2):
                    fterm_copy(t, i).start()


        @pl.when(jnp.logical_and(has_left2, lax.rem(chip, 4) != 0))
        def _():
            for t in range(2):
                fterm_copy(t, h).start()

        for t in range(2):
            other_send[t, h] = own_terms[t, h, half(1 - core)].astype(jnp.bfloat16)

        for t in range(2):
            outs_copy(t, h).start()
            other_copy(t, h).start()
            (o_out, qg_out)[t][:, columns(core, h)] = outs[t, h, half(core)]
        return carry

    lax.fori_loop(0, heads, one_head, 0)
    @pl.when(jnp.logical_and(has_left2, lax.rem(chip, 4) == 0))
    def _():
        for i in (3,):
            for t in range(2):
                fterm_copy(t, i).start()

    for h in range(heads):
        send_nterm(h)

    for h in range(heads):
        for t in range(2):
            outs_copy(t, h).wait_recv()
            (o_out, qg_out)[t][:, columns(1 - core, h)] = outs_other[t, h]
            other_copy(t, h).wait_recv()

    for h in range(heads):
        for t in range(2):
            for c in range(2):
                j = c * heads + h

                @pl.when(has_right)
                def _():
                    remote(
                        near_send.at[t, h, half(c)],
                        near_got.at[t, j],
                        nterm_ssem.at[t, h, c],
                        nterm_rsem.at[t, j],
                        left,
                        core,
                    ).wait_recv()

                mine = own_terms[t, h, half(core)]
                other = other_got[t, h].astype(jnp.float32)
                term = jnp.where(core == c, mine, other)
                (kg_out, vg_out)[t][:, j * D : (j + 1) * D] = (
                    term + near_got[t, j].astype(jnp.float32)
                ).astype(jnp.bfloat16)

    half_copy().wait_send()
    for offset in (0, 1, -1):
        rows_to(offset, lambda offset, c: rows_copy(offset, c).wait_send())

    @pl.when(inner)
    def _():
        past_copy(1).wait_send()
        past_copy(-1).wait_send()

    for h in range(heads):
        for t in range(4):
            own_copy(t, h).wait_send()
        for t in range(2):
            outs_copy(t, h).wait_send()
            other_copy(t, h).wait_send()

    @pl.when(has_right)
    def _():
        for h in range(heads):
            for t in range(2):
                for c in range(2):
                    near_copy(h, c, t).wait_send()

    @pl.when(jnp.logical_and(has_left, has_right))
    def _():
        for h in range(heads):
            for t in range(2):
                for c in range(2):
                    far_copy(h, c, t).wait_send()

    @pl.when(has_left2)
    def _():
        for h in range(heads):
            for t in range(2):
                fterm_copy(t, h).wait_send()

    @pl.when(has_left)
    def _():
        for h in range(heads):
            for t in range(2):
                for c in range(2):
                    nterm_copy(t, h, c).wait_send()


def write_kernel(*refs):
    sems = refs[-1]
    n = (len(refs) - 1) // 2
    copies = [pltpu.make_async_copy(refs[i], refs[n + i], sems.at[i]) for i in range(n)]
    for copy in copies:
        copy.start()
    for copy in copies:
        copy.wait()


def solution(mesh):
    n_chip = mesh.shape["seq"] // 2

    def body(queries, keys, values, grad_out, doc_ids, loss_mask):
        rows, width = queries.shape
        heads = width // HEAD_DIM // 2
        D = HEAD_DIM
        bf16, f32 = jnp.bfloat16, jnp.float32
        dma = pltpu.SemaphoreType.DMA
        shape = jax.ShapeDtypeStruct((rows, width), bf16)
        vmem = pltpu.VMEM
        held = pl.pallas_call(
            functools.partial(kernel, n_chip, rows, heads),
            out_shape=(pltpu.VMEM((rows, width), bf16),) * 4,
            in_specs=[pl.BlockSpec(memory_space=pl.ANY)] * 6,
            out_specs=(pl.BlockSpec(memory_space=pltpu.VMEM),) * 4,
            scratch_shapes=[
                vmem((2, rows, width), bf16),
                vmem((2, 1, 64), jnp.int32),
                vmem((4, heads, 2 * rows, D), bf16),
                vmem((2, heads, 2 * rows, D), bf16),
                vmem((2, heads, 2 * rows, D), bf16),
                vmem((20, 1, 128), jnp.int32),
                vmem((2 * rows, 6 * rows), f32),
                vmem((2 * rows, 128), f32),
                vmem((2, heads, 2 * rows, D), bf16),
                vmem((2, heads, rows, D), bf16),
                vmem((2, heads, 2 * rows, D), f32),
                vmem((2, heads, 2 * rows, D), f32),
                vmem((2, heads, rows, D), bf16),
                vmem((2, heads, rows, D), bf16),
                vmem((2, heads, 2 * rows, D), bf16),
                vmem((2, heads, 2 * rows, D), bf16),
                vmem((2, heads, 2 * rows, D), bf16),
                vmem((2, 2 * heads, rows, D), bf16),
                dma((4, heads)),
                dma((2,)),
                dma((2,)),
                dma((4, heads)),
                dma((4, heads)),
                dma((heads, 2, 2)),
                dma((heads, 2, 2)),
                dma((heads, 2, 2)),
                dma((heads, 2, 2)),
                dma((1,)),
                dma((1,)),
                dma((3, 2)),
                dma((3, 2)),
                dma((2,)),
                dma((2,)),
                dma((2, heads)),
                dma((2, heads)),
                dma((2, heads)),
                dma((2, heads)),
                dma((2, heads)),
                dma((2, heads)),
                dma((2, heads, 2)),
                dma((2, 2 * heads)),
            ],
            compiler_params=pltpu.CompilerParams(
                collective_id=0, has_side_effects=True, vmem_limit_bytes=60 * 1024 * 1024
            ),
        )(queries, keys, values, grad_out, doc_ids.reshape(1, -1), loss_mask.reshape(1, -1))
        return pl.pallas_call(
            write_kernel,
            out_shape=(shape,) * 4,
            in_specs=[pl.BlockSpec(memory_space=pltpu.VMEM)] * 4,
            out_specs=(pl.BlockSpec(memory_space=pl.ANY),) * 4,
            scratch_shapes=[dma((4,))],
        )(*(pltpu.with_memory_space_constraint(x, pltpu.VMEM) for x in held))

    return jax.shard_map(
        body,
        mesh=mesh,
        in_specs=(P("seq", "head"),) * 4 + (P(("seq", "head")),) * 2,
        out_specs=(P("seq", "head"),) * 4,
        check_vma=False,
    )
```

```python
import functools
import math

import jax
import jax.numpy as jnp
from jax import lax
from jax.experimental import pallas as pl
from jax.experimental.pallas import tpu as pltpu
from jax.sharding import PartitionSpec as P

HEAD_DIM = 128
MASKED = -1e30
SCALE = 1.0 / math.sqrt(HEAD_DIM)
MESH = pl.DeviceIdType.MESH
NN = (((1,), (0,)), ((), ()))
NT = (((1,), (1,)), ((), ()))
TN = (((0,), (0,)), ((), ()))


def dot(a, b, dims):
    return lax.dot_general(a, b, dims, preferred_element_type=jnp.float32)


def kernel(
    n_chip,
    rows,
    heads,
    q_in,
    k_in,
    v_in,
    g_in,
    ids_in,
    mask_in,
    o_out,
    qg_out,
    kg_out,
    vg_out,
    kv_mine,
    ids_mask,
    own,
    near,
    far,
    meta,
    bias,
    weight,
    outs,
    outs_other,
    own_terms,
    near_terms,
    other_send,
    other_got,
    far_send,
    far_got,
    near_send,
    near_got,
    load_sem,
    kv_sem,
    ids_sem,
    own_ssem,
    own_rsem,
    near_ssem,
    near_rsem,
    far_ssem,
    far_rsem,
    half_ssem,
    half_rsem,
    rows_ssem,
    rows_rsem,
    past_ssem,
    past_rsem,
    outs_ssem,
    outs_rsem,
    other_ssem,
    other_rsem,
    fterm_ssem,
    fterm_rsem,
    nterm_ssem,
    nterm_rsem,
):
    D = HEAD_DIM
    me = lax.axis_index("seq")
    hd = lax.axis_index("head")
    chip, core = me // 2, lax.rem(me, 2)
    right, left = lax.rem(chip + 1, n_chip), lax.rem(chip + n_chip - 1, n_chip)
    ins = (q_in, k_in, v_in, g_in)

    has_left, has_left2 = chip >= 1, chip >= 2
    has_right, has_right2 = chip <= n_chip - 2, chip <= n_chip - 3
    exists = {-2: has_left2, -1: has_left, 1: has_right, 2: has_right2}

    def at_chip(offset):
        return lax.rem(chip + n_chip + offset, n_chip)

    def where_chip(offset, act):
        if offset == 0:
            act()
        else:
            pl.when(exists[offset])(act)

    def half(which):
        return pl.ds(pl.multiple_of(which * rows, rows), rows)

    def columns(which, h):
        return pl.ds(pl.multiple_of((which * heads + h) * D, D), D)

    def remote(src, dst, ssem, rsem, to_chip, to_core, to_hd=None):
        return pltpu.make_async_remote_copy(
            src_ref=src,
            dst_ref=dst,
            send_sem=ssem,
            recv_sem=rsem,
            device_id=(to_chip * 2 + to_core, hd if to_hd is None else to_hd),
            device_id_type=MESH,
        )

    barrier = pltpu.get_barrier_semaphore()

    def greet(to_chip, to_core, to_hd):
        pl.semaphore_signal(barrier, inc=1, device_id=(to_chip * 2 + to_core, to_hd), device_id_type=MESH)

    for offset in (-1, 1):

        @functools.partial(where_chip, offset)
        def _(offset=offset):
            for c in range(2):
                greet(at_chip(offset), c, hd)

    greet(chip, 1 - core, hd)
    greet(chip, core, 1 - hd)

    def kv_load(t):
        return pltpu.make_async_copy(ins[1 + t], kv_mine.at[t], kv_sem.at[t])

    def ids_load(t):
        return pltpu.make_async_copy((ids_in, mask_in)[t], ids_mask.at[t], ids_sem.at[t])

    for t in range(2):
        ids_load(t).start()
        kv_load(t).start()

    def load(t, h):
        return pltpu.make_async_copy(
            ins[t].at[:, columns(core, h)], own.at[t, h, half(core)], load_sem.at[t, h]
        )

    for t in range(4):
        for h in range(heads):
            load(t, h).start()

    @pl.when(jnp.logical_not(has_left))
    def _():
        near[...] = jnp.zeros_like(near)

    @pl.when(jnp.logical_not(has_left2))
    def _():
        far[...] = jnp.zeros_like(far)

    @pl.when(jnp.logical_not(has_right))
    def _():
        near_got[...] = jnp.zeros_like(near_got)

    @pl.when(jnp.logical_not(jnp.logical_and(has_left, has_right)))
    def _():
        far_got[...] = jnp.zeros_like(far_got)

    for offset in (-2, -1, 1, 2):

        @pl.when(jnp.logical_not(exists[offset]))
        def _(offset=offset):
            for c in range(2):
                meta[(2 + offset) * 4 + c * 2] = jnp.full((1, 128), -2, jnp.int32)
                meta[(2 + offset) * 4 + c * 2 + 1] = jnp.zeros((1, 128), jnp.int32)

    for t in range(2):
        ids_load(t).wait()
    packed = ids_mask[0] * 2 + ids_mask[1]
    wide = jnp.concatenate([packed, packed], axis=1)
    lane = lax.broadcasted_iota(jnp.int32, (1, 128), 1)
    wide = jnp.where((lane // 64) == hd, wide, 0)
    meta[8 + core * 2 + hd] = wide

    for t in range(2):
        kv_load(t).wait()
    there = exists[-1].astype(jnp.int32) + exists[1].astype(jnp.int32)
    pl.semaphore_wait(barrier, 2 + 2 * there)

    def near_copy(h, c, t):
        return remote(
            kv_mine.at[t, :, columns(c, h)],
            near.at[t, h, half(core)],
            near_ssem.at[h, c, t],
            near_rsem.at[h, core, t],
            right,
            c,
        )

    def near_arrival(h, c, t):
        return remote(
            near.at[t, h, half(c)], near.at[t, h, half(c)], near_ssem.at[h, c, t], near_rsem.at[h, c, t], right, core
        )

    def far_copy(h, c, t):
        return remote(
            near.at[t, h, half(c)],
            far.at[t, h, half(c)],
            far_ssem.at[h, c, t],
            far_rsem.at[h, c, t],
            right,
            core,
        )

    def send_near(h):
        @pl.when(has_right)
        def _():
            for t in range(2):
                for c in range(2):
                    near_copy(h, c, t).start()

    def relay(h):
        @pl.when(has_left)
        def _():
            for t in range(2):
                for c in range(2):
                    near_arrival(h, c, t).wait_recv()

                    @pl.when(has_right)
                    def _():
                        far_copy(h, c, t).start()

    def own_copy(t, h):
        return remote(
            ins[t].at[:, columns(1 - core, h)],
            own.at[t, h, half(core)],
            own_ssem.at[t, h],
            own_rsem.at[t, h],
            chip,
            1 - core,
        )

    def half_copy():
        mine = meta.at[8 + core * 2 + hd]
        return remote(mine, mine, half_ssem.at[0], half_rsem.at[0], chip, core, 1 - hd)

    def rows_copy(offset, c):
        return remote(
            meta.at[pl.ds(8 + core * 2, 2)],
            meta.at[pl.ds((2 - offset) * 4 + core * 2, 2)],
            rows_ssem.at[1 + offset, c],
            rows_rsem.at[1 - offset, core],
            at_chip(offset),
            c,
        )

    def rows_arrival(offset, c):
        rows_there = meta.at[pl.ds((2 + offset) * 4 + c * 2, 2)]
        return remote(rows_there, rows_there, rows_ssem.at[1 + offset, c], rows_rsem.at[1 + offset, c], chip, 1 - core)

    def past_copy(offset):
        return remote(
            meta.at[pl.ds((2 - offset) * 4, 4)],
            meta.at[pl.ds((2 - 2 * offset) * 4, 4)],
            past_ssem.at[(1 - offset) // 2],
            past_rsem.at[(1 - offset) // 2],
            at_chip(offset),
            core,
        )

    def rows_to(offset, act):
        if offset == 0:
            act(0, 1 - core)
        else:

            @pl.when(exists[offset])
            def _():
                for c in range(2):
                    act(offset, c)

    inner = jnp.logical_and(has_left, has_right)

    half_copy().start()
    send_near(0)
    send_near(1)
    half_copy().wait_recv()
    for offset in (0, 1, -1):
        rows_to(offset, lambda offset, c: rows_copy(offset, c).start())
    for h in range(heads):
        for t in range(4):
            own_copy(t, h).start()
    send_near(2)
    relay(0)
    for offset in (0, 1, -1):
        rows_to(offset, lambda offset, c: rows_arrival(offset, c).wait_recv())

    @pl.when(inner)
    def _():
        past_copy(1).start()
        past_copy(-1).start()

    send_near(3)
    for h in range(1, heads):
        relay(h)

    @pl.when(has_left2)
    def _():
        past_copy(1).wait_recv()

    @pl.when(has_right2)
    def _():
        past_copy(-1).wait_recv()

    def row_of(place):
        return meta[4 * (place // 2) + 2 * (place % 2)] + meta[4 * (place // 2) + 2 * (place % 2) + 1]

    key_rows = [row_of(place) for place in range(10)]
    key_docs = [r // 2 for r in key_rows]
    key_loss = [(r - 2 * (r // 2)).astype(jnp.float32) for r in key_rows]
    for part in range(2):
        mine = jnp.broadcast_to(key_rows[4 + part].astype(jnp.float32), (128, 128)).T.astype(jnp.int32)
        doc_q = mine // 2
        loss_q = (mine - 2 * doc_q).astype(jnp.float32)
        count = jnp.zeros((128, 128), jnp.float32)
        for place in range(10):
            same = doc_q == key_docs[place]
            count = count + jnp.where(same, key_loss[place], 0.0)
            if place < 6:
                if place == 4 + part:
                    q_at = lax.broadcasted_iota(jnp.int32, (128, 128), 0)
                    k_at = lax.broadcasted_iota(jnp.int32, (128, 128), 1)
                    same = jnp.logical_and(same, k_at <= q_at)
                if place > 4 + part:
                    block = jnp.full((128, 128), MASKED, jnp.float32)
                else:
                    block = jnp.where(same, 0.0, MASKED)
                bias[part * 128 : part * 128 + 128, place * 128 : place * 128 + 128] = block
        count = jnp.sum(count, axis=1, keepdims=True)
        weight[part * 128 : part * 128 + 128, :] = loss_q * float(rows) / jnp.maximum(count, float(rows // 8))

    for t in range(4):
        for h in range(heads):
            load(t, h).wait()
            remote(
                own.at[t, h, half(1 - core)],
                own.at[t, h, half(1 - core)],
                own_ssem.at[t, h],
                own_rsem.at[t, h],
                chip,
                1 - core,
            ).wait_recv()

    def outs_copy(t, h):
        return remote(
            outs.at[t, h, half(1 - core)],
            outs_other.at[t, h],
            outs_ssem.at[t, h],
            outs_rsem.at[t, h],
            chip,
            1 - core,
        )

    def other_copy(t, h):
        return remote(
            other_send.at[t, h], other_got.at[t, h], other_ssem.at[t, h], other_rsem.at[t, h], chip, 1 - core
        )

    def fterm_copy(t, h):
        return remote(far_send.at[t, h], far_got.at[t, h], fterm_ssem.at[t, h], fterm_rsem.at[t, h], left, core)

    def nterm_copy(t, h, c):
        return remote(
            near_send.at[t, h, half(c)],
            near_got.at[t, core * heads + h],
            nterm_ssem.at[t, h, c],
            nterm_rsem.at[t, core * heads + h],
            left,
            c,
        )

    def send_nterm(h):
        @pl.when(jnp.logical_and(has_left, has_right))
        def _():
            for t in range(2):
                fterm_copy(t, h).wait_recv()

        @pl.when(has_left)
        def _():
            for t in range(2):
                near_send[t, h] = (near_terms[t, h] + far_got[t, h].astype(jnp.float32)).astype(jnp.bfloat16)
            for t in range(2):
                for c in range(2):
                    nterm_copy(t, h, c).start()

    def one_head(h, carry):
        @pl.when(has_left2)
        def _():
            for t in range(2):
                for c in range(2):
                    far_copy(h, c, t).wait_recv()

        q, g = own[0, h], (weight[...] * own[3, h].astype(jnp.float32)).astype(jnp.bfloat16)
        ks = (far[0, h], near[0, h], own[1, h])
        vs = (far[1, h], near[1, h], own[2, h])
        width = 2 * rows
        scores = [dot(q, ks[b], NT) * SCALE + bias[:, b * width : (b + 1) * width] for b in range(3)]
        top = jnp.max(functools.reduce(jnp.maximum, scores), axis=1, keepdims=True)
        prob = [jnp.exp(s - top) for s in scores]
        total = jnp.sum(prob[0] + prob[1] + prob[2], axis=1, keepdims=True)
        inverse = 1.0 / total
        prob = [p * inverse for p in prob]
        prob_half = [p.astype(jnp.bfloat16) for p in prob]
        attended = sum(dot(prob_half[b], vs[b], NN) for b in range(3)).astype(jnp.bfloat16)
        outs[0, h] = attended
        delta = jnp.sum(g.astype(jnp.float32) * attended.astype(jnp.float32), axis=1, keepdims=True)
        score_grad = [
            (prob[b] * (dot(g, vs[b], NT) - delta) * SCALE).astype(jnp.bfloat16) for b in range(3)
        ]
        far_send[0, h] = dot(score_grad[0], q, TN).astype(jnp.bfloat16)
        far_send[1, h] = dot(prob_half[0], g, TN).astype(jnp.bfloat16)
        outs[1, h] = sum(dot(score_grad[b], ks[b], NN) for b in range(3)).astype(jnp.bfloat16)
        near_terms[0, h] = dot(score_grad[1], q, TN)
        near_terms[1, h] = dot(prob_half[1], g, TN)
        own_terms[0, h] = dot(score_grad[2], q, TN)
        own_terms[1, h] = dot(prob_half[2], g, TN)

        @pl.when(has_left2)
        def _():
            for t in range(2):
                fterm_copy(t, h).start()

        for t in range(2):
            other_send[t, h] = own_terms[t, h, half(1 - core)].astype(jnp.bfloat16)

        for t in range(2):
            outs_copy(t, h).start()
            other_copy(t, h).start()
            (o_out, qg_out)[t][:, columns(core, h)] = outs[t, h, half(core)]
        return carry

    lax.fori_loop(0, heads, one_head, 0)
    for h in range(heads):
        send_nterm(h)

    for h in range(heads):
        for t in range(2):
            outs_copy(t, h).wait_recv()
            (o_out, qg_out)[t][:, columns(1 - core, h)] = outs_other[t, h]
            other_copy(t, h).wait_recv()

    for h in range(heads):
        for t in range(2):
            for c in range(2):
                j = c * heads + h

                @pl.when(has_right)
                def _():
                    remote(
                        near_send.at[t, h, half(c)],
                        near_got.at[t, j],
                        nterm_ssem.at[t, h, c],
                        nterm_rsem.at[t, j],
                        left,
                        core,
                    ).wait_recv()

                mine = own_terms[t, h, half(core)]
                other = other_got[t, h].astype(jnp.float32)
                term = jnp.where(core == c, mine, other)
                (kg_out, vg_out)[t][:, j * D : (j + 1) * D] = (
                    term + near_got[t, j].astype(jnp.float32)
                ).astype(jnp.bfloat16)

    half_copy().wait_send()
    for offset in (0, 1, -1):
        rows_to(offset, lambda offset, c: rows_copy(offset, c).wait_send())

    @pl.when(inner)
    def _():
        past_copy(1).wait_send()
        past_copy(-1).wait_send()

    for h in range(heads):
        for t in range(4):
            own_copy(t, h).wait_send()
        for t in range(2):
            outs_copy(t, h).wait_send()
            other_copy(t, h).wait_send()

    @pl.when(has_right)
    def _():
        for h in range(heads):
            for t in range(2):
                for c in range(2):
                    near_copy(h, c, t).wait_send()

    @pl.when(jnp.logical_and(has_left, has_right))
    def _():
        for h in range(heads):
            for t in range(2):
                for c in range(2):
                    far_copy(h, c, t).wait_send()

    @pl.when(has_left2)
    def _():
        for h in range(heads):
            for t in range(2):
                fterm_copy(t, h).wait_send()

    @pl.when(has_left)
    def _():
        for h in range(heads):
            for t in range(2):
                for c in range(2):
                    nterm_copy(t, h, c).wait_send()


def write_kernel(*refs):
    sems = refs[-1]
    n = (len(refs) - 1) // 2
    copies = [pltpu.make_async_copy(refs[i], refs[n + i], sems.at[i]) for i in range(n)]
    for copy in copies:
        copy.start()
    for copy in copies:
        copy.wait()


def solution(mesh):
    n_chip = mesh.shape["seq"] // 2

    def body(queries, keys, values, grad_out, doc_ids, loss_mask):
        rows, width = queries.shape
        heads = width // HEAD_DIM // 2
        D = HEAD_DIM
        bf16, f32 = jnp.bfloat16, jnp.float32
        dma = pltpu.SemaphoreType.DMA
        shape = jax.ShapeDtypeStruct((rows, width), bf16)
        vmem = pltpu.VMEM
        held = pl.pallas_call(
            functools.partial(kernel, n_chip, rows, heads),
            out_shape=(pltpu.VMEM((rows, width), bf16),) * 4,
            in_specs=[pl.BlockSpec(memory_space=pl.ANY)] * 6,
            out_specs=(pl.BlockSpec(memory_space=pltpu.VMEM),) * 4,
            scratch_shapes=[
                vmem((2, rows, width), bf16),
                vmem((2, 1, 64), jnp.int32),
                vmem((4, heads, 2 * rows, D), bf16),
                vmem((2, heads, 2 * rows, D), bf16),
                vmem((2, heads, 2 * rows, D), bf16),
                vmem((20, 1, 128), jnp.int32),
                vmem((2 * rows, 6 * rows), f32),
                vmem((2 * rows, 128), f32),
                vmem((2, heads, 2 * rows, D), bf16),
                vmem((2, heads, rows, D), bf16),
                vmem((2, heads, 2 * rows, D), f32),
                vmem((2, heads, 2 * rows, D), f32),
                vmem((2, heads, rows, D), bf16),
                vmem((2, heads, rows, D), bf16),
                vmem((2, heads, 2 * rows, D), bf16),
                vmem((2, heads, 2 * rows, D), bf16),
                vmem((2, heads, 2 * rows, D), bf16),
                vmem((2, 2 * heads, rows, D), bf16),
                dma((4, heads)),
                dma((2,)),
                dma((2,)),
                dma((4, heads)),
                dma((4, heads)),
                dma((heads, 2, 2)),
                dma((heads, 2, 2)),
                dma((heads, 2, 2)),
                dma((heads, 2, 2)),
                dma((1,)),
                dma((1,)),
                dma((3, 2)),
                dma((3, 2)),
                dma((2,)),
                dma((2,)),
                dma((2, heads)),
                dma((2, heads)),
                dma((2, heads)),
                dma((2, heads)),
                dma((2, heads)),
                dma((2, heads)),
                dma((2, heads, 2)),
                dma((2, 2 * heads)),
            ],
            compiler_params=pltpu.CompilerParams(
                collective_id=0, has_side_effects=True, vmem_limit_bytes=60 * 1024 * 1024
            ),
        )(queries, keys, values, grad_out, doc_ids.reshape(1, -1), loss_mask.reshape(1, -1))
        return pl.pallas_call(
            write_kernel,
            out_shape=(shape,) * 4,
            in_specs=[pl.BlockSpec(memory_space=pltpu.VMEM)] * 4,
            out_specs=(pl.BlockSpec(memory_space=pl.ANY),) * 4,
            scratch_shapes=[dma((4,))],
        )(*(pltpu.with_memory_space_constraint(x, pltpu.VMEM) for x in held))

    return jax.shard_map(
        body,
        mesh=mesh,
        in_specs=(P("seq", "head"),) * 4 + (P(("seq", "head")),) * 2,
        out_specs=(P("seq", "head"),) * 4,
        check_vma=False,
    )
```

```python
import functools
import math

import jax
import jax.numpy as jnp
from jax import lax
from jax.experimental import pallas as pl
from jax.experimental.pallas import tpu as pltpu
from jax.sharding import PartitionSpec as P

HEAD_DIM = 128
MASKED = -1e30
SCALE = 1.0 / math.sqrt(HEAD_DIM)
MESH = pl.DeviceIdType.MESH
NN = (((1,), (0,)), ((), ()))
NT = (((1,), (1,)), ((), ()))
TN = (((0,), (0,)), ((), ()))


def dot(a, b, dims):
    return lax.dot_general(a, b, dims, preferred_element_type=jnp.float32)


def kernel(
    n_chip,
    rows,
    heads,
    q_in,
    k_in,
    v_in,
    g_in,
    ids_in,
    mask_in,
    o_out,
    qg_out,
    kg_out,
    vg_out,
    kv_mine,
    ids_mask,
    own,
    near,
    far,
    meta,
    bias,
    weight,
    outs,
    outs_other,
    own_terms,
    near_terms,
    other_send,
    other_got,
    far_send,
    far_got,
    near_send,
    near_got,
    load_sem,
    kv_sem,
    ids_sem,
    own_ssem,
    own_rsem,
    near_ssem,
    near_rsem,
    far_ssem,
    far_rsem,
    half_ssem,
    half_rsem,
    rows_ssem,
    rows_rsem,
    past_ssem,
    past_rsem,
    outs_ssem,
    outs_rsem,
    other_ssem,
    other_rsem,
    fterm_ssem,
    fterm_rsem,
    nterm_ssem,
    nterm_rsem,
):
    D = HEAD_DIM
    me = lax.axis_index("seq")
    hd = lax.axis_index("head")
    chip, core = me // 2, lax.rem(me, 2)
    right, left = lax.rem(chip + 1, n_chip), lax.rem(chip + n_chip - 1, n_chip)
    ins = (q_in, k_in, v_in, g_in)

    has_left, has_left2 = chip >= 1, chip >= 2
    has_right, has_right2 = chip <= n_chip - 2, chip <= n_chip - 3
    exists = {-2: has_left2, -1: has_left, 1: has_right, 2: has_right2}

    def at_chip(offset):
        return lax.rem(chip + n_chip + offset, n_chip)

    def where_chip(offset, act):
        if offset == 0:
            act()
        else:
            pl.when(exists[offset])(act)

    def half(which):
        return pl.ds(pl.multiple_of(which * rows, rows), rows)

    def columns(which, h):
        return pl.ds(pl.multiple_of((which * heads + h) * D, D), D)

    def remote(src, dst, ssem, rsem, to_chip, to_core, to_hd=None):
        return pltpu.make_async_remote_copy(
            src_ref=src,
            dst_ref=dst,
            send_sem=ssem,
            recv_sem=rsem,
            device_id=(to_chip * 2 + to_core, hd if to_hd is None else to_hd),
            device_id_type=MESH,
        )

    barrier = pltpu.get_barrier_semaphore()

    def greet(to_chip, to_core, to_hd):
        pl.semaphore_signal(barrier, inc=1, device_id=(to_chip * 2 + to_core, to_hd), device_id_type=MESH)

    for offset in (-1, 1):

        @functools.partial(where_chip, offset)
        def _(offset=offset):
            for c in range(2):
                greet(at_chip(offset), c, hd)

    greet(chip, 1 - core, hd)
    greet(chip, core, 1 - hd)

    def kv_load(t):
        return pltpu.make_async_copy(ins[1 + t], kv_mine.at[t], kv_sem.at[t])

    def ids_load(t):
        return pltpu.make_async_copy((ids_in, mask_in)[t], ids_mask.at[t], ids_sem.at[t])

    for t in range(2):
        ids_load(t).start()
        kv_load(t).start()

    def load(t, h):
        return pltpu.make_async_copy(
            ins[t].at[:, columns(core, h)], own.at[t, h, half(core)], load_sem.at[t, h]
        )

    for t in range(4):
        for h in range(heads):
            load(t, h).start()

    @pl.when(jnp.logical_not(has_left))
    def _():
        near[...] = jnp.zeros_like(near)

    @pl.when(jnp.logical_not(has_left2))
    def _():
        far[...] = jnp.zeros_like(far)

    @pl.when(jnp.logical_not(has_right))
    def _():
        near_got[...] = jnp.zeros_like(near_got)

    @pl.when(jnp.logical_not(jnp.logical_and(has_left, has_right)))
    def _():
        far_got[...] = jnp.zeros_like(far_got)

    for offset in (-2, -1, 1, 2):

        @pl.when(jnp.logical_not(exists[offset]))
        def _(offset=offset):
            for c in range(2):
                meta[(2 + offset) * 4 + c * 2] = jnp.full((1, 128), -2, jnp.int32)
                meta[(2 + offset) * 4 + c * 2 + 1] = jnp.zeros((1, 128), jnp.int32)

    for t in range(2):
        ids_load(t).wait()
    packed = ids_mask[0] * 2 + ids_mask[1]
    wide = jnp.concatenate([packed, packed], axis=1)
    lane = lax.broadcasted_iota(jnp.int32, (1, 128), 1)
    wide = jnp.where((lane // 64) == hd, wide, 0)
    meta[8 + core * 2 + hd] = wide

    for t in range(2):
        kv_load(t).wait()
    there = exists[-1].astype(jnp.int32) + exists[1].astype(jnp.int32)
    pl.semaphore_wait(barrier, 2 + 2 * there)

    def near_copy(h, c, t):
        return remote(
            kv_mine.at[t, :, columns(c, h)],
            near.at[t, h, half(core)],
            near_ssem.at[h, c, t],
            near_rsem.at[h, core, t],
            right,
            c,
        )

    def near_arrival(h, c, t):
        return remote(
            near.at[t, h, half(c)], near.at[t, h, half(c)], near_ssem.at[h, c, t], near_rsem.at[h, c, t], right, core
        )

    def far_copy(h, c, t):
        return remote(
            near.at[t, h, half(c)],
            far.at[t, h, half(c)],
            far_ssem.at[h, c, t],
            far_rsem.at[h, c, t],
            right,
            core,
        )

    def send_near(h):
        @pl.when(has_right)
        def _():
            for t in range(2):
                for c in range(2):
                    near_copy(h, c, t).start()

    def relay(h):
        @pl.when(has_left)
        def _():
            for t in range(2):
                for c in range(2):
                    near_arrival(h, c, t).wait_recv()

                    @pl.when(has_right)
                    def _():
                        far_copy(h, c, t).start()

    def own_copy(t, h):
        return remote(
            ins[t].at[:, columns(1 - core, h)],
            own.at[t, h, half(core)],
            own_ssem.at[t, h],
            own_rsem.at[t, h],
            chip,
            1 - core,
        )

    def half_copy():
        mine = meta.at[8 + core * 2 + hd]
        return remote(mine, mine, half_ssem.at[0], half_rsem.at[0], chip, core, 1 - hd)

    def rows_copy(offset, c):
        return remote(
            meta.at[pl.ds(8 + core * 2, 2)],
            meta.at[pl.ds((2 - offset) * 4 + core * 2, 2)],
            rows_ssem.at[1 + offset, c],
            rows_rsem.at[1 - offset, core],
            at_chip(offset),
            c,
        )

    def rows_arrival(offset, c):
        rows_there = meta.at[pl.ds((2 + offset) * 4 + c * 2, 2)]
        return remote(rows_there, rows_there, rows_ssem.at[1 + offset, c], rows_rsem.at[1 + offset, c], chip, 1 - core)

    def past_copy(offset):
        return remote(
            meta.at[pl.ds((2 - offset) * 4, 4)],
            meta.at[pl.ds((2 - 2 * offset) * 4, 4)],
            past_ssem.at[(1 - offset) // 2],
            past_rsem.at[(1 - offset) // 2],
            at_chip(offset),
            core,
        )

    def rows_to(offset, act):
        if offset == 0:
            act(0, 1 - core)
        else:

            @pl.when(exists[offset])
            def _():
                for c in range(2):
                    act(offset, c)

    inner = jnp.logical_and(has_left, has_right)

    half_copy().start()
    send_near(0)
    send_near(1)
    half_copy().wait_recv()
    for offset in (0, 1, -1):
        rows_to(offset, lambda offset, c: rows_copy(offset, c).start())
    for h in range(heads):
        for t in range(4):
            own_copy(t, h).start()
    send_near(2)
    send_near(3)
    relay(0)
    for offset in (0, 1, -1):
        rows_to(offset, lambda offset, c: rows_arrival(offset, c).wait_recv())

    @pl.when(inner)
    def _():
        past_copy(1).start()
        past_copy(-1).start()

    for h in range(1, heads):
        relay(h)

    @pl.when(has_left2)
    def _():
        past_copy(1).wait_recv()

    @pl.when(has_right2)
    def _():
        past_copy(-1).wait_recv()

    def row_of(place):
        return meta[4 * (place // 2) + 2 * (place % 2)] + meta[4 * (place // 2) + 2 * (place % 2) + 1]

    key_rows = [row_of(place) for place in range(10)]
    key_docs = [r // 2 for r in key_rows]
    key_loss = [(r - 2 * (r // 2)).astype(jnp.float32) for r in key_rows]
    for part in range(2):
        mine = jnp.broadcast_to(key_rows[4 + part].astype(jnp.float32), (128, 128)).T.astype(jnp.int32)
        doc_q = mine // 2
        loss_q = (mine - 2 * doc_q).astype(jnp.float32)
        count = jnp.zeros((128, 128), jnp.float32)
        for place in range(10):
            same = doc_q == key_docs[place]
            count = count + jnp.where(same, key_loss[place], 0.0)
            if place < 6:
                if place == 4 + part:
                    q_at = lax.broadcasted_iota(jnp.int32, (128, 128), 0)
                    k_at = lax.broadcasted_iota(jnp.int32, (128, 128), 1)
                    same = jnp.logical_and(same, k_at <= q_at)
                if place > 4 + part:
                    block = jnp.full((128, 128), MASKED, jnp.float32)
                else:
                    block = jnp.where(same, 0.0, MASKED)
                bias[part * 128 : part * 128 + 128, place * 128 : place * 128 + 128] = block
        count = jnp.sum(count, axis=1, keepdims=True)
        weight[part * 128 : part * 128 + 128, :] = loss_q * float(rows) / jnp.maximum(count, float(rows // 8))

    for t in range(4):
        for h in range(heads):
            load(t, h).wait()
            remote(
                own.at[t, h, half(1 - core)],
                own.at[t, h, half(1 - core)],
                own_ssem.at[t, h],
                own_rsem.at[t, h],
                chip,
                1 - core,
            ).wait_recv()

    def outs_copy(t, h):
        return remote(
            outs.at[t, h, half(1 - core)],
            outs_other.at[t, h],
            outs_ssem.at[t, h],
            outs_rsem.at[t, h],
            chip,
            1 - core,
        )

    def other_copy(t, h):
        return remote(
            other_send.at[t, h], other_got.at[t, h], other_ssem.at[t, h], other_rsem.at[t, h], chip, 1 - core
        )

    def fterm_copy(t, h):
        return remote(far_send.at[t, h], far_got.at[t, h], fterm_ssem.at[t, h], fterm_rsem.at[t, h], left, core)

    def nterm_copy(t, h, c):
        return remote(
            near_send.at[t, h, half(c)],
            near_got.at[t, core * heads + h],
            nterm_ssem.at[t, h, c],
            nterm_rsem.at[t, core * heads + h],
            left,
            c,
        )

    def send_nterm(h):
        @pl.when(jnp.logical_and(has_left, has_right))
        def _():
            for t in range(2):
                fterm_copy(t, h).wait_recv()

        @pl.when(has_left)
        def _():
            for t in range(2):
                near_send[t, h] = (near_terms[t, h] + far_got[t, h].astype(jnp.float32)).astype(jnp.bfloat16)
            for t in range(2):
                for c in range(2):
                    nterm_copy(t, h, c).start()

    def one_head(h, carry):
        @pl.when(has_left2)
        def _():
            for t in range(2):
                for c in range(2):
                    far_copy(h, c, t).wait_recv()

        q, g = own[0, h], (weight[...] * own[3, h].astype(jnp.float32)).astype(jnp.bfloat16)
        ks = (far[0, h], near[0, h], own[1, h])
        vs = (far[1, h], near[1, h], own[2, h])
        width = 2 * rows
        scores = [dot(q, ks[b], NT) * SCALE + bias[:, b * width : (b + 1) * width] for b in range(3)]
        top = jnp.max(functools.reduce(jnp.maximum, scores), axis=1, keepdims=True)
        prob = [jnp.exp(s - top) for s in scores]
        total = jnp.sum(prob[0] + prob[1] + prob[2], axis=1, keepdims=True)
        inverse = 1.0 / total
        prob = [p * inverse for p in prob]
        prob_half = [p.astype(jnp.bfloat16) for p in prob]
        attended = sum(dot(prob_half[b], vs[b], NN) for b in range(3)).astype(jnp.bfloat16)
        outs[0, h] = attended
        delta = jnp.sum(g.astype(jnp.float32) * attended.astype(jnp.float32), axis=1, keepdims=True)
        score_grad = [
            (prob[b] * (dot(g, vs[b], NT) - delta) * SCALE).astype(jnp.bfloat16) for b in range(3)
        ]
        far_send[0, h] = dot(score_grad[0], q, TN).astype(jnp.bfloat16)
        far_send[1, h] = dot(prob_half[0], g, TN).astype(jnp.bfloat16)
        outs[1, h] = sum(dot(score_grad[b], ks[b], NN) for b in range(3)).astype(jnp.bfloat16)
        near_terms[0, h] = dot(score_grad[1], q, TN)
        near_terms[1, h] = dot(prob_half[1], g, TN)
        own_terms[0, h] = dot(score_grad[2], q, TN)
        own_terms[1, h] = dot(prob_half[2], g, TN)

        @pl.when(has_left2)
        def _():
            for t in range(2):
                fterm_copy(t, h).start()

        for t in range(2):
            other_send[t, h] = own_terms[t, h, half(1 - core)].astype(jnp.bfloat16)

        for t in range(2):
            outs_copy(t, h).start()
            other_copy(t, h).start()
            (o_out, qg_out)[t][:, columns(core, h)] = outs[t, h, half(core)]
        return carry

    lax.fori_loop(0, heads, one_head, 0)
    for h in range(heads):
        send_nterm(h)

    for h in range(heads):
        for t in range(2):
            outs_copy(t, h).wait_recv()
            (o_out, qg_out)[t][:, columns(1 - core, h)] = outs_other[t, h]
            other_copy(t, h).wait_recv()

    for h in range(heads):
        for t in range(2):
            for c in range(2):
                j = c * heads + h

                @pl.when(has_right)
                def _():
                    remote(
                        near_send.at[t, h, half(c)],
                        near_got.at[t, j],
                        nterm_ssem.at[t, h, c],
                        nterm_rsem.at[t, j],
                        left,
                        core,
                    ).wait_recv()

                mine = own_terms[t, h, half(core)]
                other = other_got[t, h].astype(jnp.float32)
                term = jnp.where(core == c, mine, other)
                (kg_out, vg_out)[t][:, j * D : (j + 1) * D] = (
                    term + near_got[t, j].astype(jnp.float32)
                ).astype(jnp.bfloat16)

    half_copy().wait_send()
    for offset in (0, 1, -1):
        rows_to(offset, lambda offset, c: rows_copy(offset, c).wait_send())

    @pl.when(inner)
    def _():
        past_copy(1).wait_send()
        past_copy(-1).wait_send()

    for h in range(heads):
        for t in range(4):
            own_copy(t, h).wait_send()
        for t in range(2):
            outs_copy(t, h).wait_send()
            other_copy(t, h).wait_send()

    @pl.when(has_right)
    def _():
        for h in range(heads):
            for t in range(2):
                for c in range(2):
                    near_copy(h, c, t).wait_send()

    @pl.when(jnp.logical_and(has_left, has_right))
    def _():
        for h in range(heads):
            for t in range(2):
                for c in range(2):
                    far_copy(h, c, t).wait_send()

    @pl.when(has_left2)
    def _():
        for h in range(heads):
            for t in range(2):
                fterm_copy(t, h).wait_send()

    @pl.when(has_left)
    def _():
        for h in range(heads):
            for t in range(2):
                for c in range(2):
                    nterm_copy(t, h, c).wait_send()


def write_kernel(*refs):
    sems = refs[-1]
    n = (len(refs) - 1) // 2
    copies = [pltpu.make_async_copy(refs[i], refs[n + i], sems.at[i]) for i in range(n)]
    for copy in copies:
        copy.start()
    for copy in copies:
        copy.wait()


def solution(mesh):
    n_chip = mesh.shape["seq"] // 2

    def body(queries, keys, values, grad_out, doc_ids, loss_mask):
        rows, width = queries.shape
        heads = width // HEAD_DIM // 2
        D = HEAD_DIM
        bf16, f32 = jnp.bfloat16, jnp.float32
        dma = pltpu.SemaphoreType.DMA
        shape = jax.ShapeDtypeStruct((rows, width), bf16)
        vmem = pltpu.VMEM
        held = pl.pallas_call(
            functools.partial(kernel, n_chip, rows, heads),
            out_shape=(pltpu.VMEM((rows, width), bf16),) * 4,
            in_specs=[pl.BlockSpec(memory_space=pl.ANY)] * 6,
            out_specs=(pl.BlockSpec(memory_space=pltpu.VMEM),) * 4,
            scratch_shapes=[
                vmem((2, rows, width), bf16),
                vmem((2, 1, 64), jnp.int32),
                vmem((4, heads, 2 * rows, D), bf16),
                vmem((2, heads, 2 * rows, D), bf16),
                vmem((2, heads, 2 * rows, D), bf16),
                vmem((20, 1, 128), jnp.int32),
                vmem((2 * rows, 6 * rows), f32),
                vmem((2 * rows, 128), f32),
                vmem((2, heads, 2 * rows, D), bf16),
                vmem((2, heads, rows, D), bf16),
                vmem((2, heads, 2 * rows, D), f32),
                vmem((2, heads, 2 * rows, D), f32),
                vmem((2, heads, rows, D), bf16),
                vmem((2, heads, rows, D), bf16),
                vmem((2, heads, 2 * rows, D), bf16),
                vmem((2, heads, 2 * rows, D), bf16),
                vmem((2, heads, 2 * rows, D), bf16),
                vmem((2, 2 * heads, rows, D), bf16),
                dma((4, heads)),
                dma((2,)),
                dma((2,)),
                dma((4, heads)),
                dma((4, heads)),
                dma((heads, 2, 2)),
                dma((heads, 2, 2)),
                dma((heads, 2, 2)),
                dma((heads, 2, 2)),
                dma((1,)),
                dma((1,)),
                dma((3, 2)),
                dma((3, 2)),
                dma((2,)),
                dma((2,)),
                dma((2, heads)),
                dma((2, heads)),
                dma((2, heads)),
                dma((2, heads)),
                dma((2, heads)),
                dma((2, heads)),
                dma((2, heads, 2)),
                dma((2, 2 * heads)),
            ],
            compiler_params=pltpu.CompilerParams(
                collective_id=0, has_side_effects=True, vmem_limit_bytes=60 * 1024 * 1024
            ),
        )(queries, keys, values, grad_out, doc_ids.reshape(1, -1), loss_mask.reshape(1, -1))
        return pl.pallas_call(
            write_kernel,
            out_shape=(shape,) * 4,
            in_specs=[pl.BlockSpec(memory_space=pltpu.VMEM)] * 4,
            out_specs=(pl.BlockSpec(memory_space=pl.ANY),) * 4,
            scratch_shapes=[dma((4,))],
        )(*(pltpu.with_memory_space_constraint(x, pltpu.VMEM) for x in held))

    return jax.shard_map(
        body,
        mesh=mesh,
        in_specs=(P("seq", "head"),) * 4 + (P(("seq", "head")),) * 2,
        out_specs=(P("seq", "head"),) * 4,
        check_vma=False,
    )
```
